256 devices in a mesh: gx: 4 (over y), gy: 16 (over z, core), gz: 4 (over x).
Axes of the slice: x: 4, y: 4, z: 8, core: 2. Of those that a mesh axis runs over, the one named last changes fastest.
Arguments:
- initial: float32 [256, 512, 1024], P('gx', 'gy', 'gz'), may hold values from -6 to 6
- right_side: float32 [256, 512, 1024], P('gx', 'gy', 'gz'), may hold values from -12 to 12
- shift_field: float32 [256, 512, 1024], P('gx', 'gy', 'gz'), may hold values from 0.5 to 8
Outputs:
- relaxed: float32 [256, 512, 1024], P('gx', 'gy', 'gz')
The draws below stay inside these ranges and needn't reach their ends.
All inputs are finite; a program needn't handle non-finite values.
Results may differ from the reference program's by a relative error of at most 0.00002.
Values sent between devices are 32-bit elements; how exact they have to be, the bound alone decides.
A program may use at most 128 MiB of HBM per device.

```python
import math
import jax
import jax.numpy as jnp

SWEEPS = 4
NX = 256
NY = 512
NZ = 1024


def levels(stream_key, extent, cuts, least, high):
    def one(position, parts):
        heights = jax.random.uniform(jax.random.fold_in(jax.random.fold_in(stream_key, 6), position), (parts,), jnp.float32, least / len(cuts), high / len(cuts))
        return jnp.repeat(jnp.exp(heights), extent[position] // parts).reshape((-1,) + (1,) * (len(extent) - position - 1))

    gain = one(*cuts[0])
    for cut in cuts[1:]:
        gain = gain * one(*cut)
    return gain


def centred(stream_key, extent, scale, limit, pieces=(), held_as=jnp.bfloat16):
    array = scale * jax.random.normal(stream_key, extent, jnp.float32)
    if pieces:
        array = array * levels(stream_key, extent, pieces, -0.22, 0.18)
    return jnp.clip(array, -limit, limit).astype(held_as)


def setup_inputs(seed: int = 0) -> dict:
    keys = jax.random.split(jax.random.key(seed), 4)
    initial = centred(keys[0], (NX, NY, NZ), 1.0, 6.0, ((0, 4), (1, 16), (2, 4)), jnp.float32)
    right_side = centred(keys[1], (NX, NY, NZ), 2.0, 12.0, ((0, 4), (1, 16), (2, 4)), jnp.float32)
    shift_field = jnp.clip(jnp.exp(math.log(8.0) - 2.7725887 * jax.random.uniform(keys[2], (NX, NY, NZ), jnp.float32) ** levels(keys[2], (NX, NY, NZ), ((0, 4), (1, 16), (2, 4)), -0.2, 0.2)), 0.5, 8.0)
    return dict(initial=initial, right_side=right_side, shift_field=shift_field)


relax_weight = 0.8


def neighbours(field):
    total = jnp.roll(field, 1, 0) + jnp.roll(field, -1, 0)
    total = total + jnp.roll(field, 1, 1) + jnp.roll(field, -1, 1)
    total = total + jnp.roll(field, 1, 2) + jnp.roll(field, -1, 2)
    return total


def reference(initial, right_side, shift_field):
    diagonal = 6.0 + shift_field
    relaxed = initial
    for sweep in range(SWEEPS):
        beside = neighbours(relaxed)
        relaxed = relaxed + relax_weight * (right_side - (diagonal * relaxed - beside)) / diagonal
    return relaxed
```

```python
import functools

import jax
import jax.numpy as jnp
from jax import lax
from jax.experimental import pallas as pl
from jax.experimental.pallas import tpu as pltpu
from jax.sharding import PartitionSpec as P

SWEEPS = 4
WEIGHT = 0.8
AXES = ("gx", "gy", "gz")
MESH = pl.DeviceIdType.MESH
LANES = 128
PAD = 8
STEP = 8


def kernel(init_ref, rhs_hbm, shift_hbm, out_hbm, field, rhs, weight, z_out, z_in, load_sem, store_sem, send_sem, recv_sem):
    _, halves, planes, rows, _ = field.shape
    nx, ny = planes - 2, rows - 2 * PAD
    peers = {}
    for axis in AXES:
        me, size = lax.axis_index(axis), lax.axis_size(axis)
        peers[axis] = (lax.rem(me + 1, size), lax.rem(me + size - 1, size))

    loads = []
    for half in range(halves):
        lanes = pl.ds(half * LANES, LANES)
        loads.append((
            pltpu.make_async_copy(init_ref.at[:, :, lanes], field.at[0, half, pl.ds(1, nx), pl.ds(PAD, ny), :], load_sem.at[half, 0]),
            pltpu.make_async_copy(shift_hbm.at[:, :, lanes], weight.at[half], load_sem.at[half, 1]),
            pltpu.make_async_copy(rhs_hbm.at[:, :, lanes], rhs.at[half], load_sem.at[half, 2]),
        ))
    for which in range(3):
        for half in range(halves):
            loads[half][which].start()

    barrier = pltpu.get_barrier_semaphore()
    for axis in AXES:
        for peer in peers[axis]:
            pl.semaphore_signal(barrier, inc=1, device_id={axis: peer}, device_id_type=MESH)

    flat = field.reshape(2, halves, planes * rows, LANES)
    lane = lax.broadcasted_iota(jnp.int32, (ny, LANES), 1)
    nothing = jnp.zeros((ny, LANES), jnp.float32)

    def exchange(slot):
        copies = []
        for axis in AXES:
            for way in range(2):
                if axis == "gx":
                    src = field.at[slot, :, nx if way == 0 else 1, pl.ds(PAD, ny), :]
                    dst = field.at[slot, :, 0 if way == 0 else nx + 1, pl.ds(PAD, ny), :]
                elif axis == "gy":
                    src = field.at[slot, :, pl.ds(1, nx), pl.ds(PAD + ny - 1 if way == 0 else PAD, 1), :]
                    dst = field.at[slot, :, pl.ds(1, nx), pl.ds(PAD - 1 if way == 0 else PAD + ny, 1), :]
                else:
                    src, dst = z_out.at[slot, way], z_in.at[slot, way]
                which = 2 * AXES.index(axis) + way
                copies.append(pltpu.make_async_remote_copy(
                    src, dst, send_sem.at[slot, which], recv_sem.at[slot, which],
                    device_id={axis: peers[axis][way]}, device_id_type=MESH))
        return copies

    def pack(x, left, right, high, low):
        high = jnp.where(lane == x, pltpu.roll(right, lax.rem(x + 1, LANES), 1), high)
        low = jnp.where(lane == x, pltpu.roll(left, x, 1), low)
        return high, low

    for half in range(halves):
        loads[half][0].wait()

    def first_faces(trip, faces):
        for j in range(STEP):
            x = trip * STEP + j
            at = pl.ds(pl.multiple_of((x + 1) * rows + PAD, 8), ny)
            faces = pack(x, flat[0, 0, at, :], flat[0, halves - 1, at, :], *faces)
        return faces

    z_out[0, 0], z_out[0, 1] = lax.fori_loop(0, nx // STEP, first_faces, (nothing, nothing))
    pl.semaphore_wait(barrier, 2 * len(AXES))
    flying = exchange(0)
    for copy in flying:
        copy.start()

    for half in range(halves):
        loads[half][1].wait()

    @pl.loop(0, nx // STEP)
    def _(trip):
        at = pl.ds(pl.multiple_of(trip * STEP, STEP), STEP)
        for half in range(halves):
            weight[half, at] = WEIGHT / (6.0 + weight[half, at])

    for half in range(halves):
        loads[half][2].wait()

    stores = []
    for sweep in range(SWEEPS):
        old, new = sweep % 2, (sweep + 1) % 2
        for copy in flying:
            copy.wait()

        def planes_of(trip, faces):
            for j in range(STEP):
                x = trip * STEP + j
                base = pl.multiple_of((x + 1) * rows, 8)
                at = pl.ds(base + PAD, ny)
                here = [flat[old, half, at, :] for half in range(halves)]
                fore = [pltpu.roll(v, 1, 1) for v in here]
                back = [pltpu.roll(v, LANES - 1, 1) for v in here]
                low = pltpu.roll(z_in[old, 0], lax.rem(LANES - x, LANES), 1)
                high = pltpu.roll(z_in[old, 1], LANES - 1 - x, 1)
                fresh = []
                for half in range(halves):
                    before = jnp.where(lane == 0, low if half == 0 else fore[half - 1], fore[half])
                    after = jnp.where(lane == LANES - 1, high if half == halves - 1 else back[half + 1], back[half])
                    beside = before + after
                    beside = beside + (flat[old, half, pl.ds(base + PAD - 1, ny), :] + flat[old, half, pl.ds(base + PAD + 1, ny), :])
                    beside = beside + (flat[old, half, pl.ds(base + PAD - rows, ny), :] + flat[old, half, pl.ds(base + PAD + rows, ny), :])
                    value = (1.0 - WEIGHT) * here[half] + weight[half, x] * (rhs[half, x] + beside)
                    flat[new, half, at, :] = value
                    fresh.append(value)
                if sweep < SWEEPS - 1:
                    faces = pack(x, fresh[0], fresh[-1], *faces)
            return faces

        faces = lax.fori_loop(0, nx // STEP, planes_of, (nothing, nothing))
        if sweep < SWEEPS - 1:
            z_out[new, 0], z_out[new, 1] = faces
            flying = exchange(new)
            for copy in flying:
                copy.start()
    for half in range(halves):
        stores.append(pltpu.make_async_copy(
            field.at[SWEEPS % 2, half, pl.ds(1, nx), pl.ds(PAD, ny), :], out_hbm.at[:, :, pl.ds(half * LANES, LANES)], store_sem.at[half]))
    for copy in stores:
        copy.start()
    for copy in stores:
        copy.wait()


def relax(initial, right_side, shift_field):
    nx, ny, nz = initial.shape
    halves = nz // LANES
    block = (halves, nx, ny, LANES)
    return pl.pallas_call(
        kernel,
        out_shape=jax.ShapeDtypeStruct(initial.shape, jnp.float32),
        in_specs=[pl.BlockSpec(memory_space=pl.ANY)] * 3,
        out_specs=pl.BlockSpec(memory_space=pl.ANY),
        scratch_shapes=[
            pltpu.VMEM((2, halves, nx + 2, ny + 2 * PAD, LANES), jnp.float32),
            pltpu.VMEM(block, jnp.float32),
            pltpu.VMEM(block, jnp.float32),
            pltpu.VMEM((2, 2, ny, LANES), jnp.float32),
            pltpu.VMEM((2, 2, ny, LANES), jnp.float32),
            pltpu.SemaphoreType.DMA((halves, 3)),
            pltpu.SemaphoreType.DMA((halves,)),
            pltpu.SemaphoreType.DMA((2, 6)),
            pltpu.SemaphoreType.DMA((2, 6)),
        ],
        compiler_params=pltpu.CompilerParams(collective_id=0, has_side_effects=True),
    )(initial, right_side, shift_field)


def solution(mesh):
    return jax.shard_map(
        relax,
        mesh=mesh,
        in_specs=(P(*AXES), P(*AXES), P(*AXES)),
        out_specs=P(*AXES),
        check_vma=False,
    )
```

```python
import jax
import jax.numpy as jnp
from jax import lax
from jax.experimental import pallas as pl
from jax.experimental.pallas import tpu as pltpu
from jax.sharding import PartitionSpec as P

SWEEPS = 4
WEIGHT = 0.8
AXES = ("gx", "gy", "gz")
MESH = pl.DeviceIdType.MESH
LANES = 128
PAD = 8
STEP = 8


def kernel(
    init_hbm, rhs_hbm, shift_hbm, out_hbm, field_a, field_b, rhs, weight, weight_y, x_in, y_in, z_in, z_out,
    load_sem, store_sem, send_sem, recv_sem,
):
    halves, planes, rows, _ = field_a.shape
    nx, ny = planes - 2, rows - PAD
    last = halves - 1
    trips = nx // STEP
    field = (field_a, field_b)
    flat = tuple(f.reshape(halves, planes * rows, LANES) for f in field)
    peers = {}
    for axis in AXES:
        me, size = lax.axis_index(axis), lax.axis_size(axis)
        peers[axis] = (lax.rem(me + 1, size), lax.rem(me + size - 1, size))
    base = lax.rem(lax.axis_index("gx"), 2) * nx

    loads = []
    for source, place in ((init_hbm, field_b.at[:, pl.ds(1, nx), pl.ds(0, ny), :]), (shift_hbm, weight), (rhs_hbm, rhs)):
        which = len(loads)
        loads.append([
            pltpu.make_async_copy(source.at[:, :, pl.ds(half * LANES, LANES)], place.at[half], load_sem.at[half, which])
            for half in range(halves)
        ])
    for group in loads:
        for copy in group:
            copy.start()

    barrier = pltpu.get_barrier_semaphore()
    for axis in AXES:
        for peer in peers[axis]:
            pl.semaphore_signal(barrier, inc=1, device_id={axis: peer}, device_id_type=MESH)

    lane = lax.broadcasted_iota(jnp.int32, (ny, LANES), 1)
    behind = jnp.where(lane == LANES - 1, 0, lane + 1)
    nothing = jnp.zeros((ny, LANES), jnp.float32)

    def plane_at(x, shift=0):
        return pl.ds(pl.multiple_of((x + 1) * rows, 8) + shift, ny)

    for f in field:
        for half in range(halves):
            f[half, 0] = jnp.zeros((rows, LANES), jnp.float32)
            f[half, nx + 1] = jnp.zeros((rows, LANES), jnp.float32)

    @pl.loop(0, trips)
    def _(trip):
        for f in field:
            for half in range(halves):
                f[half, pl.ds(trip * STEP + 1, STEP), pl.ds(ny, PAD), :] = jnp.zeros((STEP, PAD, LANES), jnp.float32)

    def exchange(slot):
        copies = []
        for axis in AXES:
            for way in range(2):
                if axis == "gx":
                    src, dst = field[slot].at[:, nx if way == 0 else 1, pl.ds(0, ny), :], x_in.at[slot, way]
                elif axis == "gy":
                    src, dst = field[slot].at[:, pl.ds(1, nx), ny - 1 if way == 0 else 0, :], y_in.at[slot, way]
                else:
                    src, dst = z_out.at[slot, way], z_in.at[slot, way]
                which = 2 * AXES.index(axis) + way
                copies.append(pltpu.make_async_remote_copy(
                    src, dst, send_sem.at[slot, which], recv_sem.at[slot, which],
                    device_id={axis: peers[axis][way]}, device_id_type=MESH))
        return copies

    def pack(skew, faces, first, final):
        return jnp.where(behind == skew, final, faces[0]), jnp.where(lane == skew, first, faces[1])

    for copy in loads[0]:
        copy.wait()

    def rotate_field(trip, faces):
        for j in range(STEP):
            x = trip * STEP + j
            turned = [pltpu.roll(flat[1][half, plane_at(x), :], base + x, 1) for half in range(halves)]
            for half in range(halves):
                flat[0][half, plane_at(x), :] = turned[half]
            faces = pack(base + x, faces, turned[0], turned[last])
        return faces

    z_out[0, 0], z_out[0, 1] = lax.fori_loop(0, trips, rotate_field, (nothing, nothing))
    pl.semaphore_wait(barrier, 2 * len(AXES))
    flying = exchange(0)
    for copy in flying:
        copy.start()

    for copy in loads[1]:
        copy.wait()

    def rotate_weight(trip, faces):
        for j in range(STEP):
            x = trip * STEP + j
            turned = [WEIGHT / (6.0 + pltpu.roll(weight[half, x], base + x, 1)) for half in range(halves)]
            for half in range(halves):
                weight[half, x] = turned[half]
            faces = pack(base + x, faces, turned[0], turned[last])
        return faces

    weight_high, weight_low = lax.fori_loop(0, trips, rotate_weight, (nothing, nothing))
    z_weight = (weight_low, weight_high)
    for copy in loads[2]:
        copy.wait()

    @pl.loop(0, trips)
    def _(trip):
        for j in range(STEP):
            x = trip * STEP + j
            for half in range(halves):
                rhs[half, x] = pltpu.roll(rhs[half, x], base + x, 1)

    flat_weight = weight.reshape(halves, nx * ny, LANES)
    for side, row in ((0, 0), (1, ny - 1)):
        for half in range(halves):
            for x in range(0, nx, 8):
                weight_y[side, half, pl.ds(x, 8)] = flat_weight[half, pl.ds(x * ny + row, 8, stride=ny), :]

    for sweep in range(SWEEPS):
        old, new = sweep % 2, (sweep + 1) % 2

        @pl.loop(0, trips)
        def _(trip):
            for j in range(STEP):
                x = trip * STEP + j
                here = [flat[old][half, plane_at(x), :] for half in range(halves)]
                at_first, at_last = lane == base + x, behind == base + x
                for half in range(halves):
                    after = jnp.where(at_first, here[half + 1] if half < last else 0.0, here[half]) + flat[old][half, plane_at(x + 1), :]
                    before = jnp.where(at_last, here[half - 1] if half > 0 else 0.0, here[half]) + flat[old][half, plane_at(x - 1), :]
                    beside = flat[old][half, plane_at(x, -1), :] + flat[old][half, plane_at(x, 1), :] + rhs[half, x]
                    beside = beside + (pltpu.roll(after, LANES - 1, 1) + pltpu.roll(before, 1, 1))
                    flat[new][half, plane_at(x), :] = (1.0 - WEIGHT) * here[half] + weight[half, x] * beside

        for copy in flying:
            copy.wait()

        for way, x, turn in ((0, 0, 1), (1, nx - 1, LANES - 1)):
            for half in range(halves):
                flat[new][half, plane_at(x), :] += weight[half, x] * pltpu.roll(x_in[old, way, half], turn, 1)
        for way, row in ((0, 0), (1, ny - 1)):
            for half in range(halves):
                for x in range(0, nx, 8):
                    at = pl.ds((x + 1) * rows + row, 8, stride=rows)
                    flat[new][half, at, :] += weight_y[way, half, pl.ds(x, 8)] * y_in[old, way, half, pl.ds(x, 8)]
        add_low = z_weight[0] * pltpu.roll(z_in[old, 0], 1, 1)
        add_high = z_weight[1] * pltpu.roll(z_in[old, 1], LANES - 1, 1)

        def corrected(x):
            at_first, at_last = lane == base + x, behind == base + x
            values = [flat[new][half, plane_at(x), :] for half in range(halves)]
            values[0] = values[0] + jnp.where(at_first, add_low, 0.0)
            values[last] = values[last] + jnp.where(at_last, add_high, 0.0)
            return values

        if sweep < SWEEPS - 1:

            def finish(trip, faces):
                for j in range(STEP):
                    x = trip * STEP + j
                    values = corrected(x)
                    for half in range(halves):
                        flat[new][half, plane_at(x), :] = values[half]
                    faces = pack(base + x, faces, values[0], values[last])
                return faces

            z_out[new, 0], z_out[new, 1] = lax.fori_loop(0, trips, finish, (nothing, nothing))
            flying = exchange(new)
            for copy in flying:
                copy.start()

    def store(trip, half):
        some = pl.multiple_of(trip * STEP, STEP)
        return pltpu.make_async_copy(
            field[old].at[half, pl.ds(some + 1, STEP), pl.ds(0, ny), :],
            out_hbm.at[pl.ds(some, STEP), :, pl.ds(half * LANES, LANES)], store_sem.at[half, trip])

    @pl.loop(0, trips)
    def _(trip):
        for j in range(STEP):
            x = trip * STEP + j
            values = corrected(x)
            for half in range(halves):
                flat[old][half, plane_at(x), :] = pltpu.roll(values[half], lax.rem(LANES - base - x, LANES), 1)
        for half in range(halves):
            store(trip, half).start()

    @pl.loop(0, trips)
    def _(trip):
        for half in range(halves):
            store(trip, half).wait()


def relax(initial, right_side, shift_field):
    nx, ny, nz = initial.shape
    halves = nz // LANES
    plane = (ny, LANES)
    field = (halves, nx + 2, ny + PAD, LANES)
    f32 = jnp.float32
    return pl.pallas_call(
        kernel,
        out_shape=jax.ShapeDtypeStruct(initial.shape, f32),
        in_specs=[pl.BlockSpec(memory_space=pl.ANY)] * 3,
        out_specs=pl.BlockSpec(memory_space=pl.ANY),
        scratch_shapes=[
            pltpu.VMEM(field, f32),
            pltpu.VMEM(field, f32),
            pltpu.VMEM((halves, nx) + plane, f32),
            pltpu.VMEM((halves, nx) + plane, f32),
            pltpu.VMEM((2, halves, nx, LANES), f32),
            pltpu.VMEM((2, 2, halves) + plane, f32),
            pltpu.VMEM((2, 2, halves, nx, LANES), f32),
            pltpu.VMEM((2, 2) + plane, f32),
            pltpu.VMEM((2, 2) + plane, f32),
            pltpu.SemaphoreType.DMA((halves, 3)),
            pltpu.SemaphoreType.DMA((halves, nx // STEP)),
            pltpu.SemaphoreType.DMA((2, 6)),
            pltpu.SemaphoreType.DMA((2, 6)),
        ],
        compiler_params=pltpu.CompilerParams(collective_id=0, has_side_effects=True),
    )(initial, right_side, shift_field)


def solution(mesh):
    return jax.shard_map(
        relax,
        mesh=mesh,
        in_specs=(P(*AXES), P(*AXES), P(*AXES)),
        out_specs=P(*AXES),
        check_vma=False,
    )
```

```python
import jax
import jax.numpy as jnp
from jax import lax
from jax.experimental import pallas as pl
from jax.experimental.pallas import tpu as pltpu
from jax.sharding import PartitionSpec as P

SWEEPS = 4
WEIGHT = 0.8
AXES = ("gx", "gy", "gz")
MESH = pl.DeviceIdType.MESH
LANES = 128
PAD = 8
STEP = 8


def kernel(
    init_hbm, rhs_hbm, shift_hbm, out, field_a, field_b, rhs, weight, weight_y, x_in, y_in, z_in, z_out,
    load_sem, send_sem, recv_sem,
):
    halves, planes, rows, _ = field_a.shape
    nx, ny = planes - 2, rows - PAD
    last = halves - 1
    trips = nx // STEP
    field = (field_a, field_b)
    flat = tuple(f.reshape(halves, planes * rows, LANES) for f in field)
    peers = {}
    for axis in AXES:
        me, size = lax.axis_index(axis), lax.axis_size(axis)
        peers[axis] = (lax.rem(me + 1, size), lax.rem(me + size - 1, size))
    base = lax.rem(lax.axis_index("gx"), 2) * nx

    loads = []
    for source, place in ((init_hbm, field_b.at[:, pl.ds(1, nx), pl.ds(0, ny), :]), (shift_hbm, weight), (rhs_hbm, rhs)):
        which = len(loads)
        loads.append([
            pltpu.make_async_copy(source.at[:, :, pl.ds(half * LANES, LANES)], place.at[half], load_sem.at[half, which])
            for half in range(halves)
        ])
    for group in loads:
        for copy in group:
            copy.start()

    barrier = pltpu.get_barrier_semaphore()
    for axis in AXES:
        for peer in peers[axis]:
            pl.semaphore_signal(barrier, inc=1, device_id={axis: peer}, device_id_type=MESH)

    lane = lax.broadcasted_iota(jnp.int32, (ny, LANES), 1)
    behind = jnp.where(lane == LANES - 1, 0, lane + 1)
    nothing = jnp.zeros((ny, LANES), jnp.float32)

    def plane_at(x, shift=0):
        return pl.ds(pl.multiple_of((x + 1) * rows, 8) + shift, ny)

    for f in field:
        for half in range(halves):
            f[half, 0] = jnp.zeros((rows, LANES), jnp.float32)
            f[half, nx + 1] = jnp.zeros((rows, LANES), jnp.float32)

    @pl.loop(0, trips)
    def _(trip):
        for f in field:
            for half in range(halves):
                f[half, pl.ds(trip * STEP + 1, STEP), pl.ds(ny, PAD), :] = jnp.zeros((STEP, PAD, LANES), jnp.float32)

    def exchange(slot):
        copies = []
        for axis in AXES:
            for way in range(2):
                if axis == "gx":
                    src, dst = field[slot].at[:, nx if way == 0 else 1, pl.ds(0, ny), :], x_in.at[slot, way]
                elif axis == "gy":
                    src, dst = field[slot].at[:, pl.ds(1, nx), ny - 1 if way == 0 else 0, :], y_in.at[slot, way]
                else:
                    src, dst = z_out.at[slot, way], z_in.at[slot, way]
                which = 2 * AXES.index(axis) + way
                copies.append(pltpu.make_async_remote_copy(
                    src, dst, send_sem.at[slot, which], recv_sem.at[slot, which],
                    device_id={axis: peers[axis][way]}, device_id_type=MESH))
        return copies

    def pack(skew, faces, first, final):
        return jnp.where(behind == skew, final, faces[0]), jnp.where(lane == skew, first, faces[1])

    for copy in loads[0]:
        copy.wait()

    def rotate_field(trip, faces):
        for j in range(STEP):
            x = trip * STEP + j
            turned = [pltpu.roll(flat[1][half, plane_at(x), :], base + x, 1) for half in range(halves)]
            for half in range(halves):
                flat[0][half, plane_at(x), :] = turned[half]
            faces = pack(base + x, faces, turned[0], turned[last])
        return faces

    z_out[0, 0], z_out[0, 1] = lax.fori_loop(0, trips, rotate_field, (nothing, nothing))
    pl.semaphore_wait(barrier, 2 * len(AXES))
    flying = exchange(0)
    for copy in flying:
        copy.start()

    for copy in loads[1]:
        copy.wait()

    def rotate_weight(trip, faces):
        for j in range(STEP):
            x = trip * STEP + j
            turned = [WEIGHT / (6.0 + pltpu.roll(weight[half, x], base + x, 1)) for half in range(halves)]
            for half in range(halves):
                weight[half, x] = turned[half]
            faces = pack(base + x, faces, turned[0], turned[last])
        return faces

    weight_high, weight_low = lax.fori_loop(0, trips, rotate_weight, (nothing, nothing))
    z_weight = (weight_low, weight_high)
    for copy in loads[2]:
        copy.wait()

    @pl.loop(0, trips)
    def _(trip):
        for j in range(STEP):
            x = trip * STEP + j
            for half in range(halves):
                rhs[half, x] = pltpu.roll(rhs[half, x], base + x, 1)

    flat_weight = weight.reshape(halves, nx * ny, LANES)
    for side, row in ((0, 0), (1, ny - 1)):
        for half in range(halves):
            for x in range(0, nx, 8):
                weight_y[side, half, pl.ds(x, 8)] = flat_weight[half, pl.ds(x * ny + row, 8, stride=ny), :]

    for sweep in range(SWEEPS):
        old, new = sweep % 2, (sweep + 1) % 2

        @pl.loop(0, trips)
        def _(trip):
            for j in range(STEP):
                x = trip * STEP + j
                here = [flat[old][half, plane_at(x), :] for half in range(halves)]
                at_first, at_last = lane == base + x, behind == base + x
                for half in range(halves):
                    after = jnp.where(at_first, here[half + 1] if half < last else 0.0, here[half]) + flat[old][half, plane_at(x + 1), :]
                    before = jnp.where(at_last, here[half - 1] if half > 0 else 0.0, here[half]) + flat[old][half, plane_at(x - 1), :]
                    beside = flat[old][half, plane_at(x, -1), :] + flat[old][half, plane_at(x, 1), :] + rhs[half, x]
                    beside = beside + (pltpu.roll(after, LANES - 1, 1) + pltpu.roll(before, 1, 1))
                    flat[new][half, plane_at(x), :] = (1.0 - WEIGHT) * here[half] + weight[half, x] * beside

        for copy in flying:
            copy.wait()

        for way, x, turn in ((0, 0, 1), (1, nx - 1, LANES - 1)):
            for half in range(halves):
                flat[new][half, plane_at(x), :] += weight[half, x] * pltpu.roll(x_in[old, way, half], turn, 1)
        for way, row in ((0, 0), (1, ny - 1)):
            for half in range(halves):
                for x in range(0, nx, 8):
                    at = pl.ds((x + 1) * rows + row, 8, stride=rows)
                    flat[new][half, at, :] += weight_y[way, half, pl.ds(x, 8)] * y_in[old, way, half, pl.ds(x, 8)]
        add_low = z_weight[0] * pltpu.roll(z_in[old, 0], 1, 1)
        add_high = z_weight[1] * pltpu.roll(z_in[old, 1], LANES - 1, 1)

        def corrected(x):
            at_first, at_last = lane == base + x, behind == base + x
            values = [flat[new][half, plane_at(x), :] for half in range(halves)]
            values[0] = values[0] + jnp.where(at_first, add_low, 0.0)
            values[last] = values[last] + jnp.where(at_last, add_high, 0.0)
            return values

        if sweep < SWEEPS - 1:

            def finish(trip, faces):
                for j in range(STEP):
                    x = trip * STEP + j
                    values = corrected(x)
                    for half in range(halves):
                        flat[new][half, plane_at(x), :] = values[half]
                    faces = pack(base + x, faces, values[0], values[last])
                return faces

            z_out[new, 0], z_out[new, 1] = lax.fori_loop(0, trips, finish, (nothing, nothing))
            flying = exchange(new)
            for copy in flying:
                copy.start()

    @pl.loop(0, trips)
    def _(trip):
        for j in range(STEP):
            x = trip * STEP + j
            values = corrected(x)
            for half in range(halves):
                out[x, :, half * LANES:(half + 1) * LANES] = pltpu.roll(values[half], lax.rem(LANES - base - x, LANES), 1)


def relax(initial, right_side, shift_field):
    nx, ny, nz = initial.shape
    halves = nz // LANES
    plane = (ny, LANES)
    field = (halves, nx + 2, ny + PAD, LANES)
    f32 = jnp.float32
    return pl.pallas_call(
        kernel,
        out_shape=jax.ShapeDtypeStruct(initial.shape, f32),
        in_specs=[pl.BlockSpec(memory_space=pltpu.HBM)] * 3,
        out_specs=pl.BlockSpec(memory_space=pltpu.VMEM),
        scratch_shapes=[
            pltpu.VMEM(field, f32),
            pltpu.VMEM(field, f32),
            pltpu.VMEM((halves, nx) + plane, f32),
            pltpu.VMEM((halves, nx) + plane, f32),
            pltpu.VMEM((2, halves, nx, LANES), f32),
            pltpu.VMEM((2, 2, halves) + plane, f32),
            pltpu.VMEM((2, 2, halves, nx, LANES), f32),
            pltpu.VMEM((2, 2) + plane, f32),
            pltpu.VMEM((2, 2) + plane, f32),
            pltpu.SemaphoreType.DMA((halves, 3)),
            pltpu.SemaphoreType.DMA((2, 6)),
            pltpu.SemaphoreType.DMA((2, 6)),
        ],
        compiler_params=pltpu.CompilerParams(collective_id=0, has_side_effects=True, vmem_limit_bytes=24 * 2**20),
    )(*(pltpu.with_memory_space_constraint(a, pltpu.HBM) for a in (initial, right_side, shift_field)))


def solution(mesh):
    return jax.shard_map(
        relax,
        mesh=mesh,
        in_specs=(P(*AXES), P(*AXES), P(*AXES)),
        out_specs=P(*AXES),
        check_vma=False,
    )
```

```python
import jax
import jax.numpy as jnp
from jax import lax
from jax.experimental import pallas as pl
from jax.experimental.pallas import tpu as pltpu
from jax.sharding import PartitionSpec as P

SWEEPS = 4
WEIGHT = 0.8
KEEP = 1.0 - WEIGHT
AXES = ("gx", "gy", "gz")
MESH = pl.DeviceIdType.MESH
LANES = 128
PAD = 8
STEP = 16


def kernel(
    init_hbm, rhs_hbm, shift_hbm, out, field_a, field_b, field_c, rhs, weight, weight_y, rhs_y, z_coef, z_out, x_in, y_in, z_in,
    x_near, x_far, y_near, y_far, z_near, z_far, xy_in, xz_in, yz_in, x_coef, y_coef, z_coef_in, x_add, y_add, z_add,
    load_sem, send_sem, recv_sem, deep_send, deep_recv, coef_send, coef_recv,
):
    halves, planes, rows, _ = field_a.shape
    nx, ny = planes - 2, rows - PAD
    last = halves - 1
    trips = nx // STEP
    field = (field_a, field_b, field_c)
    flat = tuple(f.reshape(halves, planes * rows, LANES) for f in field)
    peers = {}
    for axis in AXES:
        me, size = lax.axis_index(axis), lax.axis_size(axis)
        peers[axis] = (lax.rem(me + 1, size), lax.rem(me + size - 1, size))
    base = lax.rem(lax.axis_index("gx"), 2) * nx
    sides = ((0, 1), (1, LANES - 1))

    loads = []
    for source, place in ((init_hbm, field_b.at[:, pl.ds(1, nx), pl.ds(0, ny), :]), (shift_hbm, weight), (rhs_hbm, rhs)):
        which = len(loads)
        loads.append([
            pltpu.make_async_copy(source.at[:, :, pl.ds(half * LANES, LANES)], place.at[half], load_sem.at[half, which])
            for half in range(halves)
        ])
    for group in loads:
        for copy in group:
            copy.start()

    barrier = pltpu.get_barrier_semaphore()
    for axis in AXES:
        for peer in peers[axis]:
            pl.semaphore_signal(barrier, inc=1, device_id={axis: peer}, device_id_type=MESH)

    lane = lax.broadcasted_iota(jnp.int32, (ny, LANES), 1)
    behind = jnp.where(lane == LANES - 1, 0, lane + 1)
    behind_two = jnp.where(behind == LANES - 1, 0, behind + 1)
    ahead = jnp.where(lane == 0, LANES - 1, lane - 1)
    nothing = jnp.zeros((ny, LANES), jnp.float32)

    def plane_at(x, shift=0):
        return pl.ds(pl.multiple_of((x + 1) * rows, 8) + shift, ny)

    def row_at(x, row):
        return pl.ds((x + 1) * rows + row, 8, stride=rows)

    for f in field[:2]:
        for half in range(halves):
            f[half, 0] = jnp.zeros((rows, LANES), jnp.float32)
            f[half, nx + 1] = jnp.zeros((rows, LANES), jnp.float32)

    @pl.loop(0, trips)
    def _(trip):
        for f in field[:2]:
            for half in range(halves):
                f[half, pl.ds(trip * STEP + 1, STEP), pl.ds(ny, PAD), :] = jnp.zeros((STEP, PAD, LANES), jnp.float32)

    edge = jnp.zeros((PAD, LANES), jnp.float32)
    for way in range(2):
        for half in range(halves):
            for ref, size in ((x_add.at[way, half], ny), (y_add.at[way, half], nx)):
                ref[pl.ds(0, PAD)] = edge
                ref[pl.ds(PAD + size, PAD)] = edge
        z_add[way, pl.ds(0, PAD)] = edge
        z_add[way, pl.ds(PAD + ny, PAD)] = edge

    def send(src, dst, sems, which, target):
        return pltpu.make_async_remote_copy(
            src, dst, sems[0].at[which], sems[1].at[which], device_id=target, device_id_type=MESH)

    def exchange(slot):
        copies = []
        for axis in AXES:
            for way in range(2):
                if axis == "gx":
                    src, dst = field[slot].at[:, nx if way == 0 else 1, pl.ds(0, ny), :], x_in.at[slot, way]
                elif axis == "gy":
                    src, dst = field[slot].at[:, pl.ds(1, nx), ny - 1 if way == 0 else 0, :], y_in.at[slot, way]
                else:
                    src, dst = z_out.at[slot, 0, way], z_in.at[slot, way]
                which = 6 * slot + 2 * AXES.index(axis) + way
                copies.append(send(src, dst, (send_sem, recv_sem), which, {axis: peers[axis][way]}))
        return copies

    def deep_exchange(slot):
        near, far, around = [], [], []
        f = field[slot]

        def add(group, src, dst, target):
            which = len(near) + len(far) + len(around)
            group.append(send(src, dst, (deep_send, deep_recv), which, target))

        for way in range(2):
            up = way == 0
            target = {axis: {axis: peers[axis][way]} for axis in AXES}
            add(near, f.at[:, nx if up else 1, pl.ds(0, ny), :], x_near.at[way, :, pl.ds(PAD, ny), :], target["gx"])
            add(near, f.at[:, pl.ds(1, nx), ny - 1 if up else 0, :], y_near.at[way, :, pl.ds(PAD, nx), :], target["gy"])
            add(near, z_out.at[slot, 0, way], z_near.at[way, pl.ds(PAD, ny), :], target["gz"])
            add(far, f.at[:, nx - 1 if up else 2, pl.ds(0, ny), :], x_far.at[way], target["gx"])
            add(far, f.at[:, pl.ds(1, nx), ny - 2 if up else 1, :], y_far.at[way], target["gy"])
            add(far, z_out.at[slot, 1, way], z_far.at[way], target["gz"])
            for other in range(2):
                row = pl.ds(ny - 1 if other == 0 else 0, 1)
                add(around, f.at[:, nx if up else 1, row, :], xy_in.at[way, other, :, pl.ds(0, 1), :],
                    {"gx": peers["gx"][way], "gy": peers["gy"][other]})
                add(around, z_out.at[slot, 0, other], xz_in.at[way, other], {"gx": peers["gx"][way], "gz": peers["gz"][other]})
                row = pl.ds(ny - 1 if up else 0, 1)
                add(around, z_out.at[slot, 0, other, row, :], yz_in.at[way, other, pl.ds(0, 1), :],
                    {"gy": peers["gy"][way], "gz": peers["gz"][other]})
        return around + near + far

    def coefficients(kind):
        copies = []
        whole, lines = ((weight, weight_y), (rhs, rhs_y))[kind]
        for way in range(2):
            for axis, src, dst in (
                ("gx", whole.at[:, nx - 1 if way == 0 else 0], x_coef.at[kind, way]),
                ("gy", lines.at[0, 1 - way], y_coef.at[kind, way]),
                ("gz", z_coef.at[kind, way], z_coef_in.at[kind, way]),
            ):
                which = 6 * kind + 2 * AXES.index(axis) + way
                copies.append(send(src, dst, (coef_send, coef_recv), which, {axis: peers[axis][way]}))
        return copies

    def pack(skew, faces, first, final):
        return jnp.where(behind == skew, final, faces[0]), jnp.where(lane == skew, first, faces[1])

    for copy in loads[0]:
        copy.wait()

    def rotate_field(trip, faces):
        for j in range(STEP):
            x = trip * STEP + j
            turned = [pltpu.roll(flat[1][half, plane_at(x), :], base + x, 1) for half in range(halves)]
            for half in range(halves):
                flat[0][half, plane_at(x), :] = turned[half]
            faces = pack(base + x, faces, turned[0], turned[last])
        return faces

    z_out[0, 0, 0], z_out[0, 0, 1] = lax.fori_loop(0, trips, rotate_field, (nothing, nothing))
    pl.semaphore_wait(barrier, 2 * len(AXES))
    flying = exchange(0)
    for copy in flying:
        copy.start()

    def second(skew):
        return ahead == skew, behind_two == skew

    for copy in loads[1]:
        copy.wait()

    def rotate_weight(trip, faces):
        for j in range(STEP):
            x = trip * STEP + j
            turned = [WEIGHT / (6.0 + pltpu.roll(weight[half, x], base + x, 1)) for half in range(halves)]
            for half in range(halves):
                weight[half, x] = turned[half]
            next_low, next_high = second(base + x)
            faces = pack(base + x, faces[:2], turned[0], turned[last]) + (
                jnp.where(next_high, turned[last], faces[2]), jnp.where(next_low, turned[0], faces[3]))
        return faces

    z_coef[0, 0], z_coef[0, 1], inner_high, inner_low = lax.fori_loop(0, trips, rotate_weight, (nothing,) * 4)
    z_coef[2, 0], z_coef[2, 1] = inner_high, inner_low

    def lines_of(values, lines, inner):
        by_row = values.reshape(halves, nx * ny, LANES)
        for side in range(2):
            row = ny - 1 - inner if side else inner
            for half in range(halves):
                for x in range(0, nx, 8):
                    lines[inner, side, half, pl.ds(x, 8)] = by_row[half, pl.ds(x * ny + row, 8, stride=ny), :]

    lines_of(weight, weight_y, 0)
    for copy in loads[2]:
        copy.wait()

    def rotate_rhs(trip, faces):
        for j in range(STEP):
            x = trip * STEP + j
            turned = [pltpu.roll(rhs[half, x], base + x, 1) for half in range(halves)]
            for half in range(halves):
                rhs[half, x] = turned[half]
            faces = pack(base + x, faces, turned[0], turned[last])
        return faces

    z_coef[1, 0], z_coef[1, 1] = lax.fori_loop(0, trips, rotate_rhs, (nothing, nothing))

    def sweep_inside(old, new):
        @pl.loop(0, trips)
        def _(trip):
            for j in range(STEP):
                x = trip * STEP + j
                here = [flat[old][half, plane_at(x), :] for half in range(halves)]
                at_first, at_last = lane == base + x, behind == base + x
                for half in range(halves):
                    after = jnp.where(at_first, here[half + 1] if half < last else 0.0, here[half]) + flat[old][half, plane_at(x + 1), :]
                    before = jnp.where(at_last, here[half - 1] if half > 0 else 0.0, here[half]) + flat[old][half, plane_at(x - 1), :]
                    beside = flat[old][half, plane_at(x, -1), :] + flat[old][half, plane_at(x, 1), :] + rhs[half, x]
                    beside = beside + (pltpu.roll(after, LANES - 1, 1) + pltpu.roll(before, 1, 1))
                    flat[new][half, plane_at(x), :] = KEEP * here[half] + weight[half, x] * beside

    for sweep in range(SWEEPS - 2):
        old, new = sweep % 2, (sweep + 1) % 2
        if sweep == 1:
            lines_of(weight, weight_y, 1)
            lines_of(rhs, rhs_y, 0)
            sent = coefficients(0) + coefficients(1)
            for copy in sent:
                copy.start()
        sweep_inside(old, new)
        for copy in flying:
            copy.wait()

        for way, turn in sides:
            x = (0, nx - 1)[way]
            for half in range(halves):
                flat[new][half, plane_at(x), :] += weight[half, x] * pltpu.roll(x_in[old, way, half], turn, 1)
        for way, _ in sides:
            for half in range(halves):
                for x in range(0, nx, 8):
                    at = row_at(x, (0, ny - 1)[way])
                    flat[new][half, at, :] += weight_y[0, way, half, pl.ds(x, 8)] * y_in[old, way, half, pl.ds(x, 8)]
        add_low = z_coef[0, 1] * pltpu.roll(z_in[old, 0], 1, 1)
        add_high = z_coef[0, 0] * pltpu.roll(z_in[old, 1], LANES - 1, 1)
        deep = sweep == SWEEPS - 3

        def finish(trip, faces):
            for j in range(STEP):
                x = trip * STEP + j
                at_first, at_last = lane == base + x, behind == base + x
                values = [flat[new][half, plane_at(x), :] for half in range(halves)]
                values[0] = values[0] + jnp.where(at_first, add_low, 0.0)
                values[last] = values[last] + jnp.where(at_last, add_high, 0.0)
                for half in range(halves):
                    flat[new][half, plane_at(x), :] = values[half]
                packed = pack(base + x, faces[:2], values[0], values[last])
                if deep:
                    next_low, next_high = second(base + x)
                    packed += (jnp.where(next_high, values[last], faces[2]), jnp.where(next_low, values[0], faces[3]))
                faces = packed
            return faces

        faces = lax.fori_loop(0, trips, finish, (nothing,) * (4 if deep else 2))
        z_out[new, 0, 0], z_out[new, 0, 1] = faces[:2]
        if deep:
            z_out[new, 1, 0], z_out[new, 1, 1] = faces[2:]
        flying = deep_exchange(new) if deep else exchange(new)
        for copy in flying:
            copy.start()

    sweep_inside(0, 1)
    sweep_inside(1, 2)
    for copy in flying + sent:
        copy.wait()

    outside = (lax.rem(base + LANES - 1, LANES), lax.rem(base + nx, LANES))

    def along_plane(buf, skew, below, above):
        sums = []
        here = [buf[half, pl.ds(PAD, ny)] for half in range(halves)]
        for half in range(halves):
            after = jnp.where(lane == skew, here[half + 1] if half < last else above, here[half])
            before = jnp.where(behind == skew, here[half - 1] if half > 0 else below, here[half])
            sums.append(
                (buf[half, pl.ds(PAD - 1, ny)] + buf[half, pl.ds(PAD + 1, ny)])
                + (pltpu.roll(after, LANES - 1, 1) + pltpu.roll(before, 1, 1)))
        return sums

    tall = lax.broadcasted_iota(jnp.int32, (nx, LANES), 1)
    plane_skew = lax.broadcasted_iota(jnp.int32, (nx, LANES), 0) + base
    tall_first = tall == plane_skew
    tall_last = jnp.where(tall == LANES - 1, 0, tall + 1) == plane_skew

    def along_lines(buf, below, above):
        sums = []
        here = [buf[half, pl.ds(PAD, nx)] for half in range(halves)]
        for half in range(halves):
            after = jnp.where(tall_first, here[half + 1] if half < last else above, here[half]) + buf[half, pl.ds(PAD + 1, nx)]
            before = jnp.where(tall_last, here[half - 1] if half > 0 else below, here[half]) + buf[half, pl.ds(PAD - 1, nx)]
            sums.append(pltpu.roll(after, LANES - 1, 1) + pltpu.roll(before, 1, 1))
        return sums

    def along_columns(buf, here):
        return (buf[pl.ds(PAD - 1, ny)] + buf[pl.ds(PAD + 1, ny)]) + (pltpu.roll(here, LANES - 1, 1) + pltpu.roll(here, 1, 1))

    for way in range(2):
        for other in range(2):
            for half in range(halves):
                line = xy_in[way, other, half, pl.ds(0, 1)]
                x_near[way, half, pl.ds((PAD - 1, PAD + ny)[other], 1)] = line
                y_near[other, half, pl.ds((PAD - 1, PAD + nx)[way], 1)] = line
            z_near[other, pl.ds((PAD - 1, PAD + ny)[way], 1)] = yz_in[way, other, pl.ds(0, 1)]

    z_total, z_inner = [], []
    for way, turn in sides:
        back = LANES - turn
        edge_x, edge_y = (0, nx - 1)[way], (0, ny - 1)[way]
        inner_x, inner_y = (1, nx - 2)[way], (1, ny - 2)[way]

        ring = along_plane(x_near.at[way], outside[way], xz_in[way, 0], xz_in[way, 1])
        for half in range(halves):
            near = x_near[way, half, pl.ds(PAD, ny)]
            beyond = ring[half] + x_coef[1, way, half]
            beyond = beyond + (pltpu.roll(x_far[way, half], turn, 1) + pltpu.roll(flat[0][half, plane_at(edge_x), :], back, 1))
            ring[half] = pltpu.roll(KEEP * near + x_coef[0, way, half] * beyond, turn, 1)
            x_add[way, half, pl.ds(PAD, ny)] = weight[half, edge_x] * pltpu.roll(near, turn, 1)
        spread = along_plane(x_add.at[way], base + edge_x, 0.0, 0.0)
        for half in range(halves):
            late = x_add[way, half, pl.ds(PAD, ny)]
            flat[2][half, plane_at(edge_x), :] += weight[half, edge_x] * (ring[half] + spread[half]) + KEEP * late
            flat[2][half, plane_at(inner_x), :] += weight[half, inner_x] * pltpu.roll(late, turn, 1)

        ring = along_lines(y_near.at[way], yz_in[way, 0, pl.ds(0, 1)], yz_in[way, 1, pl.ds(0, 1)])
        for half in range(halves):
            near = y_near[way, half, pl.ds(PAD, nx)]
            own = jnp.concatenate([flat[0][half, row_at(x, edge_y), :] for x in range(0, nx, 8)], axis=0)
            beyond = ring[half] + y_coef[1, way, half] + (y_far[way, half] + own)
            ring[half] = KEEP * near + y_coef[0, way, half] * beyond
            y_add[way, half, pl.ds(PAD, nx)] = weight_y[0, way, half] * near
        spread = along_lines(y_add.at[way], 0.0, 0.0)
        for half in range(halves):
            late = y_add[way, half, pl.ds(PAD, nx)]
            outer = weight_y[0, way, half] * (ring[half] + spread[half]) + KEEP * late
            inner = weight_y[1, way, half] * late
            for x in range(0, nx, 8):
                flat[2][half, row_at(x, edge_y), :] += outer[x:x + 8]
                flat[2][half, row_at(x, inner_y), :] += inner[x:x + 8]

        place = (behind, lane)[way]
        near = z_near[way, pl.ds(PAD, ny)]
        full = jnp.where(place == outside[0], xz_in[0, way], jnp.where(place == outside[1], xz_in[1, way], near))
        beyond = along_columns(z_near.at[way], full) + z_coef_in[1, way]
        beyond = beyond + (pltpu.roll(z_far[way], turn, 1) + pltpu.roll(z_out[0, 0, 1 - way], back, 1))
        ring = pltpu.roll(KEEP * near + z_coef_in[0, way] * beyond, turn, 1)
        late = z_coef[0, 1 - way] * pltpu.roll(near, turn, 1)
        z_add[way, pl.ds(PAD, ny)] = late
        z_total.append(z_coef[0, 1 - way] * (ring + along_columns(z_add.at[way], late)) + KEEP * late)
        z_inner.append(z_coef[2, 1 - way] * pltpu.roll(late, turn, 1))

    @pl.loop(0, trips)
    def _(trip):
        for j in range(STEP):
            x = trip * STEP + j
            next_low, next_high = second(base + x)
            turn = LANES - base - x if j else lax.rem(LANES - base - x, LANES)
            values = [flat[2][half, plane_at(x), :] for half in range(halves)]
            values[0] = values[0] + jnp.where(lane == base + x, z_total[0], jnp.where(next_low, z_inner[0], 0.0))
            values[last] = values[last] + jnp.where(behind == base + x, z_total[1], jnp.where(next_high, z_inner[1], 0.0))
            for half in range(halves):
                out[x, :, half * LANES:(half + 1) * LANES] = pltpu.roll(values[half], turn, 1)


def relax(initial, right_side, shift_field):
    nx, ny, nz = initial.shape
    halves = nz // LANES
    plane, padded = (ny, LANES), (ny + 2 * PAD, LANES)
    layer = (nx, LANES)
    field = (halves, nx + 2, ny + PAD, LANES)
    shapes = [
        field, field, field, (halves, nx) + plane, (halves, nx) + plane, (2, 2, halves) + layer, (1, 2, halves) + layer,
        (3, 2) + plane, (2, 2, 2) + plane,
        (2, 2, halves) + plane, (2, 2, halves) + layer, (2, 2) + plane,
        (2, halves) + padded, (2, halves) + plane, (2, halves, nx + 2 * PAD, LANES), (2, halves) + layer, (2,) + padded, (2,) + plane,
        (2, 2, halves, PAD, LANES), (2, 2) + plane, (2, 2, PAD, LANES),
        (2, 2, halves) + plane, (2, 2, halves) + layer, (2, 2) + plane,
        (2, halves) + padded, (2, halves, nx + 2 * PAD, LANES), (2,) + padded,
    ]
    dma = pltpu.SemaphoreType.DMA
    return pl.pallas_call(
        kernel,
        out_shape=jax.ShapeDtypeStruct(initial.shape, jnp.float32),
        in_specs=[pl.BlockSpec(memory_space=pltpu.HBM)] * 3,
        out_specs=pl.BlockSpec(memory_space=pltpu.VMEM),
        scratch_shapes=[pltpu.VMEM(shape, jnp.float32) for shape in shapes]
        + [dma((halves, 3)), dma((12,)), dma((12,)), dma((24,)), dma((24,)), dma((12,)), dma((12,))],
        compiler_params=pltpu.CompilerParams(collective_id=0, has_side_effects=True, vmem_limit_bytes=32 * 2**20),
    )(*(pltpu.with_memory_space_constraint(a, pltpu.HBM) for a in (initial, right_side, shift_field)))


def solution(mesh):
    return jax.shard_map(
        relax,
        mesh=mesh,
        in_specs=(P(*AXES), P(*AXES), P(*AXES)),
        out_specs=P(*AXES),
        check_vma=False,
    )
```

```python
import jax
import jax.numpy as jnp
from jax import lax
from jax.experimental import pallas as pl
from jax.experimental.pallas import tpu as pltpu
from jax.sharding import PartitionSpec as P

SWEEPS = 4
WEIGHT = 0.8
KEEP = 1.0 - WEIGHT
AXES = ("gx", "gy", "gz")
MESH = pl.DeviceIdType.MESH
LANES = 128
PAD = 8
STEP = 16
INNER, OUTER = 20, 32


def kernel(
    init_hbm, rhs_hbm, shift_hbm, out, field_a, field_b, field_c, rhs, weight, weight_y, rhs_y, z_coef, z_out, x_in, y_in, z_in,
    x_near, x_far, y_near, y_far, z_near, z_far, xy_in, xz_in, yz_in, x_coef, y_coef, z_coef_in, x_add, y_add, z_add,
    load_sem, send_sem, recv_sem,
):
    halves, planes, rows, _ = field_a.shape
    nx, ny = planes - 2, rows - PAD
    last = halves - 1
    trips = nx // STEP
    field = (field_a, field_b, field_c)
    flat = tuple(f.reshape(halves, planes * rows, LANES) for f in field)
    peers = {}
    for axis in AXES:
        me, size = lax.axis_index(axis), lax.axis_size(axis)
        peers[axis] = (lax.rem(me + 1, size), lax.rem(me + size - 1, size))
    base = lax.rem(lax.axis_index("gx"), 2) * nx
    sides = ((0, 1), (1, LANES - 1))

    all_planes = rhs.reshape(halves * nx, ny, LANES)
    face, layer_planes = halves, halves * nx // ny

    def wait_planes(sem, count):
        some = all_planes.at[pl.ds(0, count)]
        pltpu.make_async_copy(some, some, sem).wait()

    def wait_lines(sem, count):
        some = all_planes.at[0, pl.ds(0, count)]
        pltpu.make_async_copy(some, some, sem).wait()

    def load_part(trip):
        some = trip * STEP
        return [
            pltpu.make_async_copy(
                init_hbm.at[pl.ds(some, STEP), :, pl.ds(half * LANES, LANES)],
                field_b.at[half, pl.ds(some + 1, STEP), pl.ds(0, ny), :], load_sem.at[trip])
            for half in range(halves)
        ]

    loads = [
        [
            pltpu.make_async_copy(source.at[:, :, pl.ds(half * LANES, LANES)], place.at[half], load_sem.at[trips + which])
            for half in range(halves)
        ]
        for which, (source, place) in enumerate(((shift_hbm, weight), (rhs_hbm, rhs)))
    ]
    for trip in range(trips):
        for copy in load_part(trip):
            copy.start()
    for group in loads:
        for copy in group:
            copy.start()
    barrier = pltpu.get_barrier_semaphore()
    for axis in AXES:
        for peer in peers[axis]:
            pl.semaphore_signal(barrier, inc=1, device_id={axis: peer}, device_id_type=MESH)

    lane = lax.broadcasted_iota(jnp.int32, (ny, LANES), 1)
    behind = jnp.where(lane == LANES - 1, 0, lane + 1)
    behind_two = jnp.where(behind == LANES - 1, 0, behind + 1)
    ahead = jnp.where(lane == 0, LANES - 1, lane - 1)
    nothing = jnp.zeros((ny, LANES), jnp.float32)
    tall = lax.broadcasted_iota(jnp.int32, (nx, LANES), 1)
    plane_skew = lax.broadcasted_iota(jnp.int32, (nx, LANES), 0) + base
    tall_first = tall == plane_skew
    tall_last = jnp.where(tall == LANES - 1, 0, tall + 1) == plane_skew
    tall_second = jnp.where(tall == 0, LANES - 1, tall - 1) == plane_skew
    tall_last_but_one = jnp.where(tall >= LANES - 2, tall - (LANES - 2), tall + 2) == plane_skew

    def plane_at(x, shift=0):
        return pl.ds(pl.multiple_of((x + 1) * rows, 8) + shift, ny)

    def row_at(x, row):
        return pl.ds((x + 1) * rows + row, 8, stride=rows)

    for f in field[:2]:
        for half in range(halves):
            f[half, 0] = jnp.zeros((rows, LANES), jnp.float32)
            f[half, nx + 1] = jnp.zeros((rows, LANES), jnp.float32)

    @pl.loop(0, trips)
    def _(trip):
        for f in field[:2]:
            for half in range(halves):
                f[half, pl.ds(trip * STEP + 1, STEP), pl.ds(ny, PAD), :] = jnp.zeros((STEP, PAD, LANES), jnp.float32)

    edge = jnp.zeros((PAD, LANES), jnp.float32)
    for way in range(2):
        for half in range(halves):
            for ref, size in ((x_add.at[way, half], ny), (y_add.at[way, half], nx)):
                ref[pl.ds(0, PAD)] = edge
                ref[pl.ds(PAD + size, PAD)] = edge
        z_add[way, pl.ds(0, PAD)] = edge
        z_add[way, pl.ds(PAD + ny, PAD)] = edge

    def send(src, dst, sent, received, target):
        pltpu.make_async_remote_copy(
            src, dst, send_sem.at[sent], recv_sem.at[received], device_id=target, device_id_type=MESH).start()

    def exchange(slot):
        for axis in AXES:
            for way in range(2):
                if axis == "gx":
                    src, dst = field[slot].at[:, nx if way == 0 else 1, pl.ds(0, ny), :], x_in.at[slot, way]
                elif axis == "gy":
                    src, dst = field[slot].at[:, pl.ds(1, nx), ny - 1 if way == 0 else 0, :], y_in.at[slot, way]
                else:
                    src, dst = z_out.at[slot, 0, way], z_in.at[slot, way]
                send(src, dst, slot, slot if axis == "gz" else 2 + slot, {axis: peers[axis][way]})

    def deep_exchange(slot):
        f = field[slot]
        for way in range(2):
            send(f.at[:, nx if way == 0 else 1, pl.ds(0, ny), :], x_near.at[way, :, pl.ds(PAD, ny), :], 2, 6, {"gx": peers["gx"][way]})
            send(f.at[:, pl.ds(1, nx), ny - 1 if way == 0 else 0, :], y_near.at[way, :, pl.ds(PAD, nx), :], 2, 6, {"gy": peers["gy"][way]})
        for way in range(2):
            send(z_out.at[slot, 0, way], z_near.at[way, pl.ds(PAD, ny), :], 2, 4, {"gz": peers["gz"][way]})
            send(z_out.at[slot, 1, way], z_far.at[way], 2, 4, {"gz": peers["gz"][way]})
            for other in range(2):
                row = pl.ds(ny - 1 if way == 0 else 0, 1)
                send(z_out.at[slot, 0, other], xz_in.at[way, other], 2, 4, {"gx": peers["gx"][way], "gz": peers["gz"][other]})
                send(z_out.at[slot, 0, other, row, :], yz_in.at[way, other, pl.ds(0, 1), :], 3, 5,
                     {"gy": peers["gy"][way], "gz": peers["gz"][other]})
                row = pl.ds(ny - 1 if other == 0 else 0, 1)
                send(f.at[:, nx if way == 0 else 1, row, :], xy_in.at[way, other, :, pl.ds(0, 1), :], 3, 5,
                     {"gx": peers["gx"][way], "gy": peers["gy"][other]})
        for way in range(2):
            send(f.at[:, nx - 1 if way == 0 else 2, pl.ds(0, ny), :], x_far.at[way], 2, 6, {"gx": peers["gx"][way]})
            send(f.at[:, pl.ds(1, nx), ny - 2 if way == 0 else 1, :], y_far.at[way], 2, 6, {"gy": peers["gy"][way]})

    def coefficients(kind):
        whole, lines = ((weight, weight_y), (rhs, rhs_y))[kind]
        for way in range(2):
            send(whole.at[:, nx - 1 if way == 0 else 0], x_coef.at[kind, way], 4, 7, {"gx": peers["gx"][way]})
            send(lines.at[0, 1 - way], y_coef.at[kind, way], 4, 7, {"gy": peers["gy"][way]})
            send(z_coef.at[kind, way], z_coef_in.at[kind, way], 4, 7, {"gz": peers["gz"][way]})

    def pack(skew, faces, first, final):
        return jnp.where(behind == skew, final, faces[0]), jnp.where(lane == skew, first, faces[1])

    def rotate_field(trip, faces):
        wait_planes(load_sem.at[trip], halves * STEP)
        for j in range(STEP):
            x = trip * STEP + j
            turned = [pltpu.roll(flat[1][half, plane_at(x), :], base + x, 1) for half in range(halves)]
            for half in range(halves):
                flat[0][half, plane_at(x), :] = turned[half]
            faces = pack(base + x, faces, turned[0], turned[last])
        return faces

    z_out[0, 0, 0], z_out[0, 0, 1] = lax.fori_loop(0, trips, rotate_field, (nothing, nothing))
    pl.semaphore_wait(barrier, 2 * len(AXES))
    exchange(0)

    def second(skew):
        return ahead == skew, behind_two == skew

    wait_planes(load_sem.at[trips], halves * nx)

    def rotate_weight(trip, faces):
        for j in range(STEP):
            x = trip * STEP + j
            turned = [WEIGHT / (6.0 + pltpu.roll(weight[half, x], base + x, 1)) for half in range(halves)]
            for half in range(halves):
                weight[half, x] = turned[half]
            next_low, next_high = second(base + x)
            faces = pack(base + x, faces[:2], turned[0], turned[last]) + (
                jnp.where(next_high, turned[last], faces[2]), jnp.where(next_low, turned[0], faces[3]))
        return faces

    z_coef[0, 0], z_coef[0, 1], inner_high, inner_low = lax.fori_loop(0, trips, rotate_weight, (nothing,) * 4)
    z_coef[2, 0], z_coef[2, 1] = inner_high, inner_low

    def lines_of(values, lines, inner):
        by_row = values.reshape(halves, nx * ny, LANES)
        for side in range(2):
            row = ny - 1 - inner if side else inner
            for half in range(halves):
                for x in range(0, nx, 8):
                    lines[inner, side, half, pl.ds(x, 8)] = by_row[half, pl.ds(x * ny + row, 8, stride=ny), :]

    lines_of(weight, weight_y, 0)
    wait_planes(load_sem.at[trips + 1], halves * nx)

    def rotate_rhs(trip, faces):
        for j in range(STEP):
            x = trip * STEP + j
            turned = [pltpu.roll(rhs[half, x], base + x, 1) for half in range(halves)]
            for half in range(halves):
                rhs[half, x] = turned[half]
            faces = pack(base + x, faces, turned[0], turned[last])
        return faces

    z_coef[1, 0], z_coef[1, 1] = lax.fori_loop(0, trips, rotate_rhs, (nothing, nothing))

    def sweep_inside(old, new):
        @pl.loop(0, trips)
        def _(trip):
            for j in range(STEP):
                x = trip * STEP + j
                here = [flat[old][half, plane_at(x), :] for half in range(halves)]
                at_first, at_last = lane == base + x, behind == base + x
                for half in range(halves):
                    after = jnp.where(at_first, here[half + 1] if half < last else 0.0, here[half]) + flat[old][half, plane_at(x + 1), :]
                    before = jnp.where(at_last, here[half - 1] if half > 0 else 0.0, here[half]) + flat[old][half, plane_at(x - 1), :]
                    beside = flat[old][half, plane_at(x, -1), :] + flat[old][half, plane_at(x, 1), :] + rhs[half, x]
                    beside = beside + (pltpu.roll(after, LANES - 1, 1) + pltpu.roll(before, 1, 1))
                    flat[new][half, plane_at(x), :] = KEEP * here[half] + weight[half, x] * beside

    for sweep in range(SWEEPS - 2):
        old, new = sweep % 2, (sweep + 1) % 2
        if sweep == 1:
            lines_of(weight, weight_y, 1)
            lines_of(rhs, rhs_y, 0)
            coefficients(0)
            coefficients(1)
        sweep_inside(old, new)
        deep = sweep == SWEEPS - 3

        wait_planes(recv_sem.at[old], 2)
        add_low = z_coef[0, 1] * pltpu.roll(z_in[old, 0], 1, 1)
        add_high = z_coef[0, 0] * pltpu.roll(z_in[old, 1], LANES - 1, 1)

        def finish(trip, faces):
            for j in range(STEP):
                x = trip * STEP + j
                at_first, at_last = lane == base + x, behind == base + x
                values = [flat[new][half, plane_at(x), :] for half in range(halves)]
                values[0] = values[0] + jnp.where(at_first, add_low, 0.0)
                values[last] = values[last] + jnp.where(at_last, add_high, 0.0)
                for half in range(halves):
                    flat[new][half, plane_at(x), :] = values[half]
                packed = pack(base + x, faces[:2], values[0], values[last])
                if deep:
                    next_low, next_high = second(base + x)
                    packed += (jnp.where(next_high, values[last], faces[2]), jnp.where(next_low, values[0], faces[3]))
                faces = packed
            return faces

        faces = list(lax.fori_loop(0, trips, finish, (nothing,) * (4 if deep else 2)))
        wait_planes(recv_sem.at[2 + old], 2 * (face + layer_planes))
        wait_planes(send_sem.at[old], 2 * (face + layer_planes) + 2)

        columns = [(behind, last, tall_last), (lane, 0, tall_first), (behind_two, last, tall_last_but_one), (ahead, 0, tall_second)]
        for way, turn in sides:
            x = (0, nx - 1)[way]
            late = [weight[half, x] * pltpu.roll(x_in[old, way, half], turn, 1) for half in range(halves)]
            for half in range(halves):
                flat[new][half, plane_at(x), :] += late[half]
            for i, (place, half, _) in enumerate(columns[:len(faces)]):
                faces[i] = faces[i] + jnp.where(place == base + x, late[half], 0.0)
        for i, packed in enumerate(faces):
            z_out[new, i // 2, i % 2] = packed
        for way, _ in sides:
            y = (0, ny - 1)[way]
            late = [weight_y[0, way, half] * y_in[old, way, half] for half in range(halves)]
            for half in range(halves):
                for x in range(0, nx, 8):
                    flat[new][half, row_at(x, y), :] += late[half][x:x + 8]
            for i, (_, half, mask) in enumerate(columns[:len(faces)]):
                z_out[new, i // 2, i % 2, pl.ds(y, 1)] += jnp.sum(jnp.where(mask, late[half], 0.0), axis=0, keepdims=True)
        if deep:
            deep_exchange(new)
        else:
            exchange(new)

    sweep_inside(0, 1)
    sweep_inside(1, 2)
    wait_planes(send_sem.at[4], 4 * (face + layer_planes) + 4)
    wait_planes(recv_sem.at[7], 4 * (face + layer_planes) + 4)
    wait_planes(recv_sem.at[4], 8)
    wait_lines(recv_sem.at[5], 4 * halves + 4)

    outside = (lax.rem(base + LANES - 1, LANES), lax.rem(base + nx, LANES))

    def along_plane(buf, skew, below, above, more_after=(0.0,) * halves, more_before=(0.0,) * halves):
        sums = []
        here = [buf[half, pl.ds(PAD, ny)] for half in range(halves)]
        for half in range(halves):
            after = jnp.where(lane == skew, here[half + 1] if half < last else above, here[half]) + more_after[half]
            before = jnp.where(behind == skew, here[half - 1] if half > 0 else below, here[half]) + more_before[half]
            sums.append(
                (buf[half, pl.ds(PAD - 1, ny)] + buf[half, pl.ds(PAD + 1, ny)])
                + (pltpu.roll(after, LANES - 1, 1) + pltpu.roll(before, 1, 1)))
        return sums

    def along_lines(buf, below, above):
        sums = []
        here = [buf[half, pl.ds(PAD, nx)] for half in range(halves)]
        for half in range(halves):
            after = jnp.where(tall_first, here[half + 1] if half < last else above, here[half]) + buf[half, pl.ds(PAD + 1, nx)]
            before = jnp.where(tall_last, here[half - 1] if half > 0 else below, here[half]) + buf[half, pl.ds(PAD - 1, nx)]
            sums.append(pltpu.roll(after, LANES - 1, 1) + pltpu.roll(before, 1, 1))
        return sums

    def along_columns(buf, here):
        return (buf[pl.ds(PAD - 1, ny)] + buf[pl.ds(PAD + 1, ny)]) + (pltpu.roll(here, LANES - 1, 1) + pltpu.roll(here, 1, 1))

    for way in range(2):
        for other in range(2):
            z_near[other, pl.ds((PAD - 1, PAD + ny)[way], 1)] = yz_in[way, other, pl.ds(0, 1)]
    z_total, z_inner = [], []
    for way, turn in sides:
        back = LANES - turn
        place = (behind, lane)[way]
        layer = z_near[way, pl.ds(PAD, ny)]
        full = jnp.where(place == outside[0], xz_in[0, way], jnp.where(place == outside[1], xz_in[1, way], layer))
        beyond = along_columns(z_near.at[way], full) + z_coef_in[1, way]
        beyond = beyond + (pltpu.roll(z_far[way], turn, 1) + pltpu.roll(z_out[0, 0, 1 - way], back, 1))
        ring = pltpu.roll(KEEP * layer + z_coef_in[0, way] * beyond, turn, 1)
        late = z_coef[0, 1 - way] * pltpu.roll(layer, turn, 1)
        z_add[way, pl.ds(PAD, ny)] = late
        z_total.append(z_coef[0, 1 - way] * (ring + along_columns(z_add.at[way], late)) + KEEP * late)
        z_inner.append(z_coef[2, 1 - way] * pltpu.roll(late, turn, 1))

    def store(x, first, turn):
        eight = slice(first, first + 8)
        skew = base + x
        values = [flat[2][half, pl.ds(pl.multiple_of((x + 1) * rows, 8) + first, 8), :] for half in range(halves)]
        values[0] = values[0] + jnp.where(
            lane[eight] == skew, z_total[0][eight], jnp.where(ahead[eight] == skew, z_inner[0][eight], 0.0))
        values[last] = values[last] + jnp.where(
            behind[eight] == skew, z_total[1][eight], jnp.where(behind_two[eight] == skew, z_inner[1][eight], 0.0))
        for half in range(halves):
            out[x, eight, half * LANES:(half + 1) * LANES] = pltpu.roll(values[half], turn, 1)

    middle = range(8, ny - 8, 8)

    @pl.loop(0, (nx - 4) // INNER)
    def _(trip):
        for j in range(INNER):
            x = trip * INNER + j + 2
            for first in middle:
                store(x, first, LANES - base - x)

    wait_planes(send_sem.at[2], 4 * (face + layer_planes) + 8)
    wait_lines(send_sem.at[3], 4 * halves + 4)
    wait_planes(recv_sem.at[6], 4 * (face + layer_planes))
    for way in range(2):
        for other in range(2):
            for half in range(halves):
                line = xy_in[way, other, half, pl.ds(0, 1)]
                x_near[way, half, pl.ds((PAD - 1, PAD + ny)[other], 1)] = line
                y_near[other, half, pl.ds((PAD - 1, PAD + nx)[way], 1)] = line
    for way, turn in sides:
        back = LANES - turn
        edge_x, edge_y = (0, nx - 1)[way], (0, ny - 1)[way]
        inner_x, inner_y = (1, nx - 2)[way], (1, ny - 2)[way]

        beyond = [x_far[way, half] for half in range(halves)]
        own = [flat[0][half, plane_at(edge_x), :] for half in range(halves)]
        ring = along_plane(
            x_near.at[way], outside[way], xz_in[way, 0], xz_in[way, 1], *((own, beyond) if way == 0 else (beyond, own)))
        for half in range(halves):
            layer = x_near[way, half, pl.ds(PAD, ny)]
            ring[half] = pltpu.roll(KEEP * layer + x_coef[0, way, half] * (ring[half] + x_coef[1, way, half]), turn, 1)
            x_add[way, half, pl.ds(PAD, ny)] = weight[half, edge_x] * pltpu.roll(layer, turn, 1)
        spread = along_plane(x_add.at[way], base + edge_x, 0.0, 0.0)
        for half in range(halves):
            late = x_add[way, half, pl.ds(PAD, ny)]
            flat[2][half, plane_at(edge_x), :] += weight[half, edge_x] * (ring[half] + spread[half]) + KEEP * late
            flat[2][half, plane_at(inner_x), :] += weight[half, inner_x] * pltpu.roll(late, turn, 1)

        ring = along_lines(y_near.at[way], yz_in[way, 0, pl.ds(0, 1)], yz_in[way, 1, pl.ds(0, 1)])
        for half in range(halves):
            layer = y_near[way, half, pl.ds(PAD, nx)]
            own = jnp.concatenate([flat[0][half, row_at(x, edge_y), :] for x in range(0, nx, 8)], axis=0)
            beyond = ring[half] + y_coef[1, way, half] + (y_far[way, half] + own)
            ring[half] = KEEP * layer + y_coef[0, way, half] * beyond
            y_add[way, half, pl.ds(PAD, nx)] = weight_y[0, way, half] * layer
        spread = along_lines(y_add.at[way], 0.0, 0.0)
        for half in range(halves):
            late = y_add[way, half, pl.ds(PAD, nx)]
            outer = weight_y[0, way, half] * (ring[half] + spread[half]) + KEEP * late
            inner = weight_y[1, way, half] * late
            for x in range(0, nx, 8):
                flat[2][half, row_at(x, edge_y), :] += outer[x:x + 8]
                flat[2][half, row_at(x, inner_y), :] += inner[x:x + 8]

    for x in (0, 1, nx - 2, nx - 1):
        for first in middle:
            store(x, first, LANES - base - x if x else lax.rem(LANES - base, LANES))

    @pl.loop(0, nx // OUTER)
    def _(trip):
        for j in range(OUTER):
            x = trip * OUTER + j
            for first in (0, ny - 8):
                store(x, first, LANES - base - x if j else lax.rem(LANES - base - x, LANES))


def relax(initial, right_side, shift_field):
    nx, ny, nz = initial.shape
    halves = nz // LANES
    plane, padded = (ny, LANES), (ny + 2 * PAD, LANES)
    layer = (nx, LANES)
    field = (halves, nx + 2, ny + PAD, LANES)
    shapes = [
        field, field, field, (halves, nx) + plane, (halves, nx) + plane, (2, 2, halves) + layer, (1, 2, halves) + layer,
        (3, 2) + plane, (2, 2, 2) + plane,
        (2, 2, halves) + plane, (2, 2, halves) + layer, (2, 2) + plane,
        (2, halves) + padded, (2, halves) + plane, (2, halves, nx + 2 * PAD, LANES), (2, halves) + layer, (2,) + padded, (2,) + plane,
        (2, 2, halves, PAD, LANES), (2, 2) + plane, (2, 2, PAD, LANES),
        (2, 2, halves) + plane, (2, 2, halves) + layer, (2, 2) + plane,
        (2, halves) + padded, (2, halves, nx + 2 * PAD, LANES), (2,) + padded,
    ]
    dma = pltpu.SemaphoreType.DMA
    return pl.pallas_call(
        kernel,
        out_shape=jax.ShapeDtypeStruct(initial.shape, jnp.float32),
        in_specs=[pl.BlockSpec(memory_space=pltpu.HBM)] * 3,
        out_specs=pl.BlockSpec(memory_space=pltpu.VMEM),
        scratch_shapes=[pltpu.VMEM(shape, jnp.float32) for shape in shapes]
        + [dma((nx // STEP + 2,)), dma((5,)), dma((8,))],
        compiler_params=pltpu.CompilerParams(collective_id=0, has_side_effects=True, vmem_limit_bytes=32 * 2**20),
    )(*(pltpu.with_memory_space_constraint(a, pltpu.HBM) for a in (initial, right_side, shift_field)))


def solution(mesh):
    return jax.shard_map(
        relax,
        mesh=mesh,
        in_specs=(P(*AXES), P(*AXES), P(*AXES)),
        out_specs=P(*AXES),
        check_vma=False,
    )
```

```python
import jax
import jax.numpy as jnp
from jax import lax
from jax.experimental import pallas as pl
from jax.experimental.pallas import tpu as pltpu
from jax.sharding import PartitionSpec as P

SWEEPS = 4
WEIGHT = 0.8
KEEP = 1.0 - WEIGHT
AXES = ("gx", "gy", "gz")
MESH = pl.DeviceIdType.MESH
LANES = 128
PAD = 8
STEP = 16
INNER, OUTER = 20, 32


def kernel(
    init_hbm, rhs_hbm, shift_hbm, out, field_a, field_b, field_c, rhs, weight, weight_y, rhs_y, z_coef, z_out, x_in, y_in, z_in,
    x_near, x_far, y_near, y_far, z_near, z_far, xy_in, xz_in, yz_in, x_coef, y_coef, z_coef_in, x_add, y_add, z_add,
    load_sem, send_sem, recv_sem,
):
    halves, planes, rows, _ = field_a.shape
    nx, ny = planes - 2, rows - PAD
    last = halves - 1
    trips = nx // STEP
    field = (field_a, field_b, field_c)
    flat = tuple(f.reshape(halves, planes * rows, LANES) for f in field)
    peers = {}
    for axis in AXES:
        me, size = lax.axis_index(axis), lax.axis_size(axis)
        peers[axis] = (lax.rem(me + 1, size), lax.rem(me + size - 1, size))
    base = lax.rem(lax.axis_index("gx"), 2) * nx
    sides = ((0, 1), (1, LANES - 1))

    barrier = pltpu.get_barrier_semaphore()
    for axis in AXES:
        for peer in peers[axis]:
            pl.semaphore_signal(barrier, inc=1, device_id={axis: peer}, device_id_type=MESH)

    all_planes = rhs.reshape(halves * nx, ny, LANES)
    face, layer_planes = halves, halves * nx // ny

    def wait_planes(sem, count):
        some = all_planes.at[pl.ds(0, count)]
        pltpu.make_async_copy(some, some, sem).wait()

    def wait_lines(sem, count):
        some = all_planes.at[0, pl.ds(0, count)]
        pltpu.make_async_copy(some, some, sem).wait()

    def load_part(trip):
        some = trip * STEP
        return [
            pltpu.make_async_copy(
                init_hbm.at[pl.ds(some, STEP), :, pl.ds(half * LANES, LANES)],
                field_b.at[half, pl.ds(some + 1, STEP), pl.ds(0, ny), :], load_sem.at[trip])
            for half in range(halves)
        ]

    loads = [
        [
            pltpu.make_async_copy(source.at[:, :, pl.ds(half * LANES, LANES)], place.at[half], load_sem.at[trips + which])
            for half in range(halves)
        ]
        for which, (source, place) in enumerate(((shift_hbm, weight), (rhs_hbm, rhs)))
    ]
    for trip in range(trips):
        for copy in load_part(trip):
            copy.start()
    for group in loads:
        for copy in group:
            copy.start()
    lane = lax.broadcasted_iota(jnp.int32, (ny, LANES), 1)
    behind = jnp.where(lane == LANES - 1, 0, lane + 1)
    behind_two = jnp.where(behind == LANES - 1, 0, behind + 1)
    ahead = jnp.where(lane == 0, LANES - 1, lane - 1)
    nothing = jnp.zeros((ny, LANES), jnp.float32)
    tall = lax.broadcasted_iota(jnp.int32, (nx, LANES), 1)
    plane_skew = lax.broadcasted_iota(jnp.int32, (nx, LANES), 0) + base
    tall_first = tall == plane_skew
    tall_last = jnp.where(tall == LANES - 1, 0, tall + 1) == plane_skew
    tall_second = jnp.where(tall == 0, LANES - 1, tall - 1) == plane_skew
    tall_last_but_one = jnp.where(tall >= LANES - 2, tall - (LANES - 2), tall + 2) == plane_skew

    def plane_at(x, shift=0):
        return pl.ds(pl.multiple_of((x + 1) * rows, 8) + shift, ny)

    def row_at(x, row):
        return pl.ds((x + 1) * rows + row, 8, stride=rows)

    for f in field[:2]:
        for half in range(halves):
            f[half, 0] = jnp.zeros((rows, LANES), jnp.float32)
            f[half, nx + 1] = jnp.zeros((rows, LANES), jnp.float32)

    @pl.loop(0, trips)
    def _(trip):
        for f in field[:2]:
            for half in range(halves):
                f[half, pl.ds(trip * STEP + 1, STEP), pl.ds(ny, PAD), :] = jnp.zeros((STEP, PAD, LANES), jnp.float32)

    edge = jnp.zeros((PAD, LANES), jnp.float32)
    for way in range(2):
        for half in range(halves):
            for ref, size in ((x_add.at[way, half], ny), (y_add.at[way, half], nx), (x_near.at[way, half], ny), (y_near.at[way, half], nx)):
                ref[pl.ds(0, PAD)] = edge
                ref[pl.ds(PAD + size, PAD)] = edge
        for ref in (z_add.at[way], z_near.at[way]):
            ref[pl.ds(0, PAD)] = edge
            ref[pl.ds(PAD + ny, PAD)] = edge

    def send(src, dst, sent, received, target):
        pltpu.make_async_remote_copy(
            src, dst, send_sem.at[sent], recv_sem.at[received], device_id=target, device_id_type=MESH).start()

    def exchange(slot):
        for axis in AXES:
            for way in range(2):
                if axis == "gx":
                    src, dst = field[slot].at[:, nx if way == 0 else 1, pl.ds(0, ny), :], x_in.at[slot, way]
                elif axis == "gy":
                    src, dst = field[slot].at[:, pl.ds(1, nx), ny - 1 if way == 0 else 0, :], y_in.at[slot, way]
                else:
                    src, dst = z_out.at[slot, 0, way], z_in.at[slot, way]
                send(src, dst, slot, slot if axis == "gz" else 2 + slot, {axis: peers[axis][way]})

    def deep_exchange(slot):
        f = field[slot]
        for way in range(2):
            send(f.at[:, nx if way == 0 else 1, pl.ds(0, ny), :], x_near.at[way, :, pl.ds(PAD, ny), :], 2, 6, {"gx": peers["gx"][way]})
            send(f.at[:, pl.ds(1, nx), ny - 1 if way == 0 else 0, :], y_near.at[way, :, pl.ds(PAD, nx), :], 2, 6, {"gy": peers["gy"][way]})
        for way in range(2):
            send(z_out.at[slot, 0, way], z_near.at[way, pl.ds(PAD, ny), :], 2, 4, {"gz": peers["gz"][way]})
            send(z_out.at[slot, 1, way], z_far.at[way], 2, 4, {"gz": peers["gz"][way]})
            for other in range(2):
                row = pl.ds(ny - 1 if way == 0 else 0, 1)
                send(z_out.at[slot, 0, other], xz_in.at[way, other], 2, 8, {"gx": peers["gx"][way], "gz": peers["gz"][other]})
                send(z_out.at[slot, 0, other, row, :], yz_in.at[way, other, pl.ds(0, 1), :], 3, 5,
                     {"gy": peers["gy"][way], "gz": peers["gz"][other]})
                row = pl.ds(ny - 1 if other == 0 else 0, 1)
                send(f.at[:, nx if way == 0 else 1, row, :], xy_in.at[way, other, :, pl.ds(0, 1), :], 3, 5,
                     {"gx": peers["gx"][way], "gy": peers["gy"][other]})
        for way in range(2):
            send(f.at[:, nx - 1 if way == 0 else 2, pl.ds(0, ny), :], x_far.at[way], 2, 6, {"gx": peers["gx"][way]})
            send(f.at[:, pl.ds(1, nx), ny - 2 if way == 0 else 1, :], y_far.at[way], 2, 6, {"gy": peers["gy"][way]})

    def coefficients(kind):
        whole, lines = ((weight, weight_y), (rhs, rhs_y))[kind]
        for way in range(2):
            send(whole.at[:, nx - 1 if way == 0 else 0], x_coef.at[kind, way], 4, 7, {"gx": peers["gx"][way]})
            send(lines.at[0, 1 - way], y_coef.at[kind, way], 4, 7, {"gy": peers["gy"][way]})
            send(z_coef.at[kind, way], z_coef_in.at[kind, way], 4, 7, {"gz": peers["gz"][way]})

    def pack(skew, faces, first, final):
        return jnp.where(behind == skew, final, faces[0]), jnp.where(lane == skew, first, faces[1])

    def rotate_field(trip, faces):
        wait_planes(load_sem.at[trip], halves * STEP)
        for j in range(STEP):
            x = trip * STEP + j
            turned = [pltpu.roll(flat[1][half, plane_at(x), :], base + x, 1) for half in range(halves)]
            for half in range(halves):
                flat[0][half, plane_at(x), :] = turned[half]
            faces = pack(base + x, faces, turned[0], turned[last])
        return faces

    z_out[0, 0, 0], z_out[0, 0, 1] = lax.fori_loop(0, trips, rotate_field, (nothing, nothing))
    pl.semaphore_wait(barrier, 2 * len(AXES))
    exchange(0)

    def second(skew):
        return ahead == skew, behind_two == skew

    wait_planes(load_sem.at[trips], halves * nx)

    def rotate_weight(trip, faces):
        for j in range(STEP):
            x = trip * STEP + j
            turned = [WEIGHT / (6.0 + pltpu.roll(weight[half, x], base + x, 1)) for half in range(halves)]
            for half in range(halves):
                weight[half, x] = turned[half]
            next_low, next_high = second(base + x)
            faces = pack(base + x, faces[:2], turned[0], turned[last]) + (
                jnp.where(next_high, turned[last], faces[2]), jnp.where(next_low, turned[0], faces[3]))
        return faces

    z_coef[0, 0], z_coef[0, 1], inner_high, inner_low = lax.fori_loop(0, trips, rotate_weight, (nothing,) * 4)
    z_coef[2, 0], z_coef[2, 1] = inner_high, inner_low

    def lines_of(values, lines, inner):
        by_row = values.reshape(halves, nx * ny, LANES)
        for side in range(2):
            row = ny - 1 - inner if side else inner
            for half in range(halves):
                for x in range(0, nx, 8):
                    lines[inner, side, half, pl.ds(x, 8)] = by_row[half, pl.ds(x * ny + row, 8, stride=ny), :]

    lines_of(weight, weight_y, 0)
    wait_planes(load_sem.at[trips + 1], halves * nx)

    def rotate_rhs(trip, faces):
        for j in range(STEP):
            x = trip * STEP + j
            turned = [pltpu.roll(rhs[half, x], base + x, 1) for half in range(halves)]
            for half in range(halves):
                rhs[half, x] = turned[half]
            faces = pack(base + x, faces, turned[0], turned[last])
        return faces

    z_coef[1, 0], z_coef[1, 1] = lax.fori_loop(0, trips, rotate_rhs, (nothing, nothing))

    def sweep_inside(old, new):
        @pl.loop(0, trips)
        def _(trip):
            for j in range(STEP):
                x = trip * STEP + j
                here = [flat[old][half, plane_at(x), :] for half in range(halves)]
                at_first, at_last = lane == base + x, behind == base + x
                for half in range(halves):
                    after = jnp.where(at_first, here[half + 1] if half < last else 0.0, here[half]) + flat[old][half, plane_at(x + 1), :]
                    before = jnp.where(at_last, here[half - 1] if half > 0 else 0.0, here[half]) + flat[old][half, plane_at(x - 1), :]
                    beside = flat[old][half, plane_at(x, -1), :] + flat[old][half, plane_at(x, 1), :] + rhs[half, x]
                    beside = beside + (pltpu.roll(after, LANES - 1, 1) + pltpu.roll(before, 1, 1))
                    flat[new][half, plane_at(x), :] = KEEP * here[half] + weight[half, x] * beside

    for sweep in range(SWEEPS - 2):
        old, new = sweep % 2, (sweep + 1) % 2
        if sweep == 1:
            wait_planes(send_sem.at[0], 2 * (face + layer_planes) + 2)
            lines_of(weight, weight_y, 1)
            lines_of(rhs, rhs_y, 0)
            coefficients(0)
            coefficients(1)
        sweep_inside(old, new)
        deep = sweep == SWEEPS - 3

        wait_planes(recv_sem.at[old], 2)
        add_low = z_coef[0, 1] * pltpu.roll(z_in[old, 0], 1, 1)
        add_high = z_coef[0, 0] * pltpu.roll(z_in[old, 1], LANES - 1, 1)

        def finish(trip, faces):
            for j in range(STEP):
                x = trip * STEP + j
                at_first, at_last = lane == base + x, behind == base + x
                values = [flat[new][half, plane_at(x), :] for half in range(halves)]
                values[0] = values[0] + jnp.where(at_first, add_low, 0.0)
                values[last] = values[last] + jnp.where(at_last, add_high, 0.0)
                for half in range(halves):
                    flat[new][half, plane_at(x), :] = values[half]
                packed = pack(base + x, faces[:2], values[0], values[last])
                if deep:
                    next_low, next_high = second(base + x)
                    packed += (jnp.where(next_high, values[last], faces[2]), jnp.where(next_low, values[0], faces[3]))
                faces = packed
            return faces

        faces = list(lax.fori_loop(0, trips, finish, (nothing,) * (4 if deep else 2)))
        wait_planes(recv_sem.at[2 + old], 2 * (face + layer_planes))

        columns = [(behind, last, tall_last), (lane, 0, tall_first), (behind_two, last, tall_last_but_one), (ahead, 0, tall_second)]
        for way, turn in sides:
            x = (0, nx - 1)[way]
            late = [weight[half, x] * pltpu.roll(x_in[old, way, half], turn, 1) for half in range(halves)]
            for half in range(halves):
                flat[new][half, plane_at(x), :] += late[half]
            for i, (place, half, _) in enumerate(columns[:len(faces)]):
                faces[i] = faces[i] + jnp.where(place == base + x, late[half], 0.0)
        for i, packed in enumerate(faces):
            z_out[new, i // 2, i % 2] = packed
        for way, _ in sides:
            y = (0, ny - 1)[way]
            late = [weight_y[0, way, half] * y_in[old, way, half] for half in range(halves)]
            for half in range(halves):
                for x in range(0, nx, 8):
                    flat[new][half, row_at(x, y), :] += late[half][x:x + 8]
            for i, (_, half, mask) in enumerate(columns[:len(faces)]):
                z_out[new, i // 2, i % 2, pl.ds(y, 1)] += jnp.sum(jnp.where(mask, late[half], 0.0), axis=0, keepdims=True)
        if deep:
            deep_exchange(new)
        else:
            exchange(new)

    wait_planes(send_sem.at[1], 2 * (face + layer_planes) + 2)
    sweep_inside(0, 1)
    sweep_inside(1, 2)
    wait_planes(recv_sem.at[7], 4 * (face + layer_planes) + 4)
    wait_planes(recv_sem.at[4], 4)

    outside = (lax.rem(base + LANES - 1, LANES), lax.rem(base + nx, LANES))

    def along_plane(buf, skew, below, above, more_after=(0.0,) * halves, more_before=(0.0,) * halves):
        sums = []
        here = [buf[half, pl.ds(PAD, ny)] for half in range(halves)]
        for half in range(halves):
            after = jnp.where(lane == skew, here[half + 1] if half < last else above, here[half]) + more_after[half]
            before = jnp.where(behind == skew, here[half - 1] if half > 0 else below, here[half]) + more_before[half]
            sums.append(
                (buf[half, pl.ds(PAD - 1, ny)] + buf[half, pl.ds(PAD + 1, ny)])
                + (pltpu.roll(after, LANES - 1, 1) + pltpu.roll(before, 1, 1)))
        return sums

    def along_lines(buf, below, above):
        sums = []
        here = [buf[half, pl.ds(PAD, nx)] for half in range(halves)]
        for half in range(halves):
            after = jnp.where(tall_first, here[half + 1] if half < last else above, here[half]) + buf[half, pl.ds(PAD + 1, nx)]
            before = jnp.where(tall_last, here[half - 1] if half > 0 else below, here[half]) + buf[half, pl.ds(PAD - 1, nx)]
            sums.append(pltpu.roll(after, LANES - 1, 1) + pltpu.roll(before, 1, 1))
        return sums

    def along_columns(buf, here):
        return (buf[pl.ds(PAD - 1, ny)] + buf[pl.ds(PAD + 1, ny)]) + (pltpu.roll(here, LANES - 1, 1) + pltpu.roll(here, 1, 1))

    z_total, z_inner = [], []
    for way, turn in sides:
        back = LANES - turn
        layer = z_near[way, pl.ds(PAD, ny)]
        beyond = along_columns(z_near.at[way], layer) + z_coef_in[1, way]
        beyond = beyond + (pltpu.roll(z_far[way], turn, 1) + pltpu.roll(z_out[0, 0, 1 - way], back, 1))
        ring = pltpu.roll(KEEP * layer + z_coef_in[0, way] * beyond, turn, 1)
        late = z_coef[0, 1 - way] * pltpu.roll(layer, turn, 1)
        z_add[way, pl.ds(PAD, ny)] = late
        z_total.append(z_coef[0, 1 - way] * (ring + along_columns(z_add.at[way], late)) + KEEP * late)
        z_inner.append(z_coef[2, 1 - way] * pltpu.roll(late, turn, 1))

    def store(x, first, turn):
        eight = slice(first, first + 8)
        skew = base + x
        values = [flat[2][half, pl.ds(pl.multiple_of((x + 1) * rows, 8) + first, 8), :] for half in range(halves)]
        values[0] = values[0] + jnp.where(
            lane[eight] == skew, z_total[0][eight], jnp.where(ahead[eight] == skew, z_inner[0][eight], 0.0))
        values[last] = values[last] + jnp.where(
            behind[eight] == skew, z_total[1][eight], jnp.where(behind_two[eight] == skew, z_inner[1][eight], 0.0))
        for half in range(halves):
            out[x, eight, half * LANES:(half + 1) * LANES] = pltpu.roll(values[half], turn, 1)

    middle = range(8, ny - 8, 8)

    @pl.loop(0, (nx - 4) // INNER)
    def _(trip):
        for j in range(INNER):
            x = trip * INNER + j + 2
            for first in middle:
                store(x, first, LANES - base - x)

    wait_planes(recv_sem.at[6], 4 * (face + layer_planes))
    for way, turn in sides:
        back = LANES - turn
        edge_x, edge_y = (0, nx - 1)[way], (0, ny - 1)[way]
        inner_x, inner_y = (1, nx - 2)[way], (1, ny - 2)[way]

        beyond = [x_far[way, half] for half in range(halves)]
        own = [flat[0][half, plane_at(edge_x), :] for half in range(halves)]
        ring = along_plane(
            x_near.at[way], outside[way], 0.0, 0.0, *((own, beyond) if way == 0 else (beyond, own)))
        for half in range(halves):
            layer = x_near[way, half, pl.ds(PAD, ny)]
            ring[half] = pltpu.roll(KEEP * layer + x_coef[0, way, half] * (ring[half] + x_coef[1, way, half]), turn, 1)
            x_add[way, half, pl.ds(PAD, ny)] = weight[half, edge_x] * pltpu.roll(layer, turn, 1)
        spread = along_plane(x_add.at[way], base + edge_x, 0.0, 0.0)
        for half in range(halves):
            late = x_add[way, half, pl.ds(PAD, ny)]
            flat[2][half, plane_at(edge_x), :] += weight[half, edge_x] * (ring[half] + spread[half]) + KEEP * late
            flat[2][half, plane_at(inner_x), :] += weight[half, inner_x] * pltpu.roll(late, turn, 1)

        ring = along_lines(y_near.at[way], 0.0, 0.0)
        for half in range(halves):
            layer = y_near[way, half, pl.ds(PAD, nx)]
            own = jnp.concatenate([flat[0][half, row_at(x, edge_y), :] for x in range(0, nx, 8)], axis=0)
            beyond = ring[half] + y_coef[1, way, half] + (y_far[way, half] + own)
            ring[half] = KEEP * layer + y_coef[0, way, half] * beyond
            y_add[way, half, pl.ds(PAD, nx)] = weight_y[0, way, half] * layer
        spread = along_lines(y_add.at[way], 0.0, 0.0)
        for half in range(halves):
            late = y_add[way, half, pl.ds(PAD, nx)]
            outer = weight_y[0, way, half] * (ring[half] + spread[half]) + KEEP * late
            inner = weight_y[1, way, half] * late
            for x in range(0, nx, 8):
                flat[2][half, row_at(x, edge_y), :] += outer[x:x + 8]
                flat[2][half, row_at(x, inner_y), :] += inner[x:x + 8]

    wait_planes(recv_sem.at[8], 4)
    wait_lines(recv_sem.at[5], 4 * halves + 4)
    row_of = lax.broadcasted_iota(jnp.int32, (ny, LANES), 0)
    for way, turn in sides:
        edge_x, edge_y = (0, nx - 1)[way], (0, ny - 1)[way]
        for other, other_turn in sides:
            half = (0, last)[other]
            place = (behind, lane)[other]

            y = (0, ny - 1)[other]
            for each in range(halves):
                line = xy_in[way, other, each, pl.ds(0, 1)]
                through = pltpu.roll(x_coef[0, way, each, pl.ds(y, 1)] * line, turn, 1)
                through = through + y_coef[0, other, each, pl.ds(edge_x, 1)] * pltpu.roll(line, turn, 1)
                flat[2][each, pl.ds((edge_x + 1) * rows + y, 1), :] += weight_y[0, other, each, pl.ds(edge_x, 1)] * through

            only = jnp.where(place == outside[way], xz_in[way, other], 0.0)
            through = pltpu.roll(x_coef[0, way, half] * pltpu.roll(only, other_turn, 1), turn, 1)
            flat[2][half, plane_at(edge_x), :] += weight[half, edge_x] * through
            through = pltpu.roll(z_coef_in[0, other] * pltpu.roll(only, turn, 1), other_turn, 1)
            z_total[other] = z_total[other] + z_coef[0, 1 - other] * through

            line = yz_in[way, other, pl.ds(0, 1)]
            through = pltpu.roll(jnp.where(row_of == edge_y, z_coef_in[0, other] * line, 0.0), other_turn, 1)
            z_total[other] = z_total[other] + z_coef[0, 1 - other] * through
            only = jnp.where((tall_last, tall_first)[other], line, 0.0)
            through = weight_y[0, way, half] * (y_coef[0, way, half] * pltpu.roll(only, other_turn, 1))
            for x in range(0, nx, 8):
                flat[2][half, row_at(x, edge_y), :] += through[x:x + 8]

    for x in (0, 1, nx - 2, nx - 1):
        for first in middle:
            store(x, first, LANES - base - x if x else lax.rem(LANES - base, LANES))

    @pl.loop(0, nx // OUTER)
    def _(trip):
        for j in range(OUTER):
            x = trip * OUTER + j
            for first in (0, ny - 8):
                store(x, first, LANES - base - x if j else lax.rem(LANES - base - x, LANES))

    wait_planes(send_sem.at[4], 4 * (face + layer_planes) + 4)
    wait_planes(send_sem.at[2], 4 * (face + layer_planes) + 8)
    wait_lines(send_sem.at[3], 4 * halves + 4)


def relax(initial, right_side, shift_field):
    nx, ny, nz = initial.shape
    halves = nz // LANES
    plane, padded = (ny, LANES), (ny + 2 * PAD, LANES)
    layer = (nx, LANES)
    field = (halves, nx + 2, ny + PAD, LANES)
    shapes = [
        field, field, field, (halves, nx) + plane, (halves, nx) + plane, (2, 2, halves) + layer, (1, 2, halves) + layer,
        (3, 2) + plane, (2, 2, 2) + plane,
        (2, 2, halves) + plane, (2, 2, halves) + layer, (2, 2) + plane,
        (2, halves) + padded, (2, halves) + plane, (2, halves, nx + 2 * PAD, LANES), (2, halves) + layer, (2,) + padded, (2,) + plane,
        (2, 2, halves, PAD, LANES), (2, 2) + plane, (2, 2, PAD, LANES),
        (2, 2, halves) + plane, (2, 2, halves) + layer, (2, 2) + plane,
        (2, halves) + padded, (2, halves, nx + 2 * PAD, LANES), (2,) + padded,
    ]
    dma = pltpu.SemaphoreType.DMA
    return pl.pallas_call(
        kernel,
        out_shape=jax.ShapeDtypeStruct(initial.shape, jnp.float32),
        in_specs=[pl.BlockSpec(memory_space=pltpu.HBM)] * 3,
        out_specs=pl.BlockSpec(memory_space=pltpu.VMEM),
        scratch_shapes=[pltpu.VMEM(shape, jnp.float32) for shape in shapes]
        + [dma((nx // STEP + 2,)), dma((5,)), dma((9,))],
        compiler_params=pltpu.CompilerParams(collective_id=0, has_side_effects=True, vmem_limit_bytes=32 * 2**20),
    )(*(pltpu.with_memory_space_constraint(a, pltpu.HBM) for a in (initial, right_side, shift_field)))


def solution(mesh):
    return jax.shard_map(
        relax,
        mesh=mesh,
        in_specs=(P(*AXES), P(*AXES), P(*AXES)),
        out_specs=P(*AXES),
        check_vma=False,
    )
```

```python
import jax
import jax.numpy as jnp
from jax import lax
from jax.experimental import pallas as pl
from jax.experimental.pallas import tpu as pltpu
from jax.sharding import PartitionSpec as P

SWEEPS = 4
WEIGHT = 0.8
KEEP = 1.0 - WEIGHT
AXES = ("gx", "gy", "gz")
MESH = pl.DeviceIdType.MESH
LANES = 128
PAD = 8
STEP = 16
INNER, OUTER = 20, 64


def kernel(
    init_hbm, rhs_hbm, shift_hbm, out, field_a, field_b, field_c, rhs, weight, weight_y, rhs_y, z_coef, z_out, x_in, y_in, z_in,
    x_near, x_far, y_near, y_far, z_near, z_far, xy_in, xz_in, yz_in, x_coef, y_coef, z_coef_in, x_add, y_add, z_add,
    load_sem, send_sem, recv_sem,
):
    halves, planes, rows, _ = field_a.shape
    nx, ny = planes - 2, rows - PAD
    last = halves - 1
    trips = nx // STEP
    field = (field_a, field_b, field_c)
    flat = tuple(f.reshape(halves, planes * rows, LANES) for f in field)
    peers = {}
    for axis in AXES:
        me, size = lax.axis_index(axis), lax.axis_size(axis)
        peers[axis] = (lax.rem(me + 1, size), lax.rem(me + size - 1, size))
    base = lax.rem(lax.axis_index("gx"), 2) * nx
    sides = ((0, 1), (1, LANES - 1))

    barrier = pltpu.get_barrier_semaphore()
    for axis in AXES:
        for peer in peers[axis]:
            pl.semaphore_signal(barrier, inc=1, device_id={axis: peer}, device_id_type=MESH)

    all_planes = rhs.reshape(halves * nx, ny, LANES)
    face, layer_planes = halves, halves * nx // ny

    def wait_planes(sem, count):
        some = all_planes.at[pl.ds(0, count)]
        pltpu.make_async_copy(some, some, sem).wait()

    def wait_lines(sem, count):
        some = all_planes.at[0, pl.ds(0, count)]
        pltpu.make_async_copy(some, some, sem).wait()

    def load_part(trip):
        some = trip * STEP
        return [
            pltpu.make_async_copy(
                init_hbm.at[pl.ds(some, STEP), :, pl.ds(half * LANES, LANES)],
                field_b.at[half, pl.ds(some + 1, STEP), pl.ds(0, ny), :], load_sem.at[trip])
            for half in range(halves)
        ]

    loads = [
        [
            pltpu.make_async_copy(source.at[:, :, pl.ds(half * LANES, LANES)], place.at[half], load_sem.at[trips + which])
            for half in range(halves)
        ]
        for which, (source, place) in enumerate(((shift_hbm, weight), (rhs_hbm, rhs)))
    ]
    for trip in range(trips):
        for copy in load_part(trip):
            copy.start()
    for group in loads:
        for copy in group:
            copy.start()
    lane = lax.broadcasted_iota(jnp.int32, (ny, LANES), 1)
    behind = jnp.where(lane == LANES - 1, 0, lane + 1)
    behind_two = jnp.where(behind == LANES - 1, 0, behind + 1)
    ahead = jnp.where(lane == 0, LANES - 1, lane - 1)
    nothing = jnp.zeros((ny, LANES), jnp.float32)
    tall = lax.broadcasted_iota(jnp.int32, (nx, LANES), 1)
    plane_skew = lax.broadcasted_iota(jnp.int32, (nx, LANES), 0) + base
    tall_first = tall == plane_skew
    tall_last = jnp.where(tall == LANES - 1, 0, tall + 1) == plane_skew
    tall_second = jnp.where(tall == 0, LANES - 1, tall - 1) == plane_skew
    tall_last_but_one = jnp.where(tall >= LANES - 2, tall - (LANES - 2), tall + 2) == plane_skew

    def plane_at(x, shift=0):
        return pl.ds(pl.multiple_of((x + 1) * rows, 8) + shift, ny)

    def row_at(x, row):
        return pl.ds((x + 1) * rows + row, 8, stride=rows)

    for f in field[:2]:
        for half in range(halves):
            f[half, 0] = jnp.zeros((rows, LANES), jnp.float32)
            f[half, nx + 1] = jnp.zeros((rows, LANES), jnp.float32)

    @pl.loop(0, trips)
    def _(trip):
        for f in field[:2]:
            for half in range(halves):
                f[half, pl.ds(trip * STEP + 1, STEP), pl.ds(ny, PAD), :] = jnp.zeros((STEP, PAD, LANES), jnp.float32)

    edge = jnp.zeros((PAD, LANES), jnp.float32)
    for way in range(2):
        for half in range(halves):
            for ref, size in ((x_add.at[way, half], ny), (y_add.at[way, half], nx), (x_near.at[way, half], ny), (y_near.at[way, half], nx)):
                ref[pl.ds(0, PAD)] = edge
                ref[pl.ds(PAD + size, PAD)] = edge
        for ref in (z_add.at[way], z_near.at[way]):
            ref[pl.ds(0, PAD)] = edge
            ref[pl.ds(PAD + ny, PAD)] = edge

    def send(src, dst, sent, received, target):
        pltpu.make_async_remote_copy(
            src, dst, send_sem.at[sent], recv_sem.at[received], device_id=target, device_id_type=MESH).start()

    def exchange(slot):
        for axis in AXES:
            for way in range(2):
                if axis == "gx":
                    src, dst = field[slot].at[:, nx if way == 0 else 1, pl.ds(0, ny), :], x_in.at[slot, way]
                elif axis == "gy":
                    src, dst = field[slot].at[:, pl.ds(1, nx), ny - 1 if way == 0 else 0, :], y_in.at[slot, way]
                else:
                    src, dst = z_out.at[slot, 0, way], z_in.at[slot, way]
                send(src, dst, slot, slot if axis == "gz" else 2 + slot, {axis: peers[axis][way]})

    def deep_exchange(slot):
        f = field[slot]
        for way in range(2):
            send(z_out.at[slot, 0, way], z_near.at[way, pl.ds(PAD, ny), :], 2, 4, {"gz": peers["gz"][way]})
            send(z_out.at[slot, 1, way], z_far.at[way], 2, 4, {"gz": peers["gz"][way]})
            for other in range(2):
                row = pl.ds(ny - 1 if way == 0 else 0, 1)
                send(z_out.at[slot, 0, other], xz_in.at[way, other], 2, 8, {"gx": peers["gx"][way], "gz": peers["gz"][other]})
                send(z_out.at[slot, 0, other, row, :], yz_in.at[way, other, pl.ds(0, 1), :], 3, 5,
                     {"gy": peers["gy"][way], "gz": peers["gz"][other]})
                row = pl.ds(ny - 1 if other == 0 else 0, 1)
                send(f.at[:, nx if way == 0 else 1, row, :], xy_in.at[way, other, :, pl.ds(0, 1), :], 3, 5,
                     {"gx": peers["gx"][way], "gy": peers["gy"][other]})
        for way in range(2):
            send(f.at[:, nx if way == 0 else 1, pl.ds(0, ny), :], x_near.at[way, :, pl.ds(PAD, ny), :], 2, 6, {"gx": peers["gx"][way]})
            send(f.at[:, pl.ds(1, nx), ny - 1 if way == 0 else 0, :], y_near.at[way, :, pl.ds(PAD, nx), :], 2, 6, {"gy": peers["gy"][way]})
        for way in range(2):
            send(f.at[:, nx - 1 if way == 0 else 2, pl.ds(0, ny), :], x_far.at[way], 2, 6, {"gx": peers["gx"][way]})
            send(f.at[:, pl.ds(1, nx), ny - 2 if way == 0 else 1, :], y_far.at[way], 2, 6, {"gy": peers["gy"][way]})

    def coefficients(kind):
        whole, lines = ((weight, weight_y), (rhs, rhs_y))[kind]
        for way in range(2):
            send(whole.at[:, nx - 1 if way == 0 else 0], x_coef.at[kind, way], 4, 7, {"gx": peers["gx"][way]})
            send(lines.at[0, 1 - way], y_coef.at[kind, way], 4, 7, {"gy": peers["gy"][way]})
            send(z_coef.at[kind, way], z_coef_in.at[kind, way], 4, 7, {"gz": peers["gz"][way]})

    def pack(skew, faces, first, final):
        return jnp.where(behind == skew, final, faces[0]), jnp.where(lane == skew, first, faces[1])

    def rotate_field(trip, faces):
        wait_planes(load_sem.at[trip], halves * STEP)
        for j in range(STEP):
            x = trip * STEP + j
            turned = [pltpu.roll(flat[1][half, plane_at(x), :], base + x, 1) for half in range(halves)]
            for half in range(halves):
                flat[0][half, plane_at(x), :] = turned[half]
            faces = pack(base + x, faces, turned[0], turned[last])
        return faces

    z_out[0, 0, 0], z_out[0, 0, 1] = lax.fori_loop(0, trips, rotate_field, (nothing, nothing))
    pl.semaphore_wait(barrier, 2 * len(AXES))
    exchange(0)

    def second(skew):
        return ahead == skew, behind_two == skew

    wait_planes(load_sem.at[trips], halves * nx)

    def rotate_weight(trip, faces):
        for j in range(STEP):
            x = trip * STEP + j
            turned = [WEIGHT / (6.0 + pltpu.roll(weight[half, x], base + x, 1)) for half in range(halves)]
            for half in range(halves):
                weight[half, x] = turned[half]
            next_low, next_high = second(base + x)
            faces = pack(base + x, faces[:2], turned[0], turned[last]) + (
                jnp.where(next_high, turned[last], faces[2]), jnp.where(next_low, turned[0], faces[3]))
        return faces

    z_coef[0, 0], z_coef[0, 1], inner_high, inner_low = lax.fori_loop(0, trips, rotate_weight, (nothing,) * 4)
    z_coef[2, 0], z_coef[2, 1] = inner_high, inner_low

    def lines_of(values, lines, inner):
        by_row = values.reshape(halves, nx * ny, LANES)
        for side in range(2):
            row = ny - 1 - inner if side else inner
            for half in range(halves):
                for x in range(0, nx, 8):
                    lines[inner, side, half, pl.ds(x, 8)] = by_row[half, pl.ds(x * ny + row, 8, stride=ny), :]

    lines_of(weight, weight_y, 0)
    wait_planes(load_sem.at[trips + 1], halves * nx)

    def rotate_rhs(trip, faces):
        for j in range(STEP):
            x = trip * STEP + j
            turned = [pltpu.roll(rhs[half, x], base + x, 1) for half in range(halves)]
            for half in range(halves):
                rhs[half, x] = turned[half]
            faces = pack(base + x, faces, turned[0], turned[last])
        return faces

    z_coef[1, 0], z_coef[1, 1] = lax.fori_loop(0, trips, rotate_rhs, (nothing, nothing))

    def sweep_inside(old, new):
        @pl.loop(0, trips)
        def _(trip):
            for j in range(STEP):
                x = trip * STEP + j
                here = [flat[old][half, plane_at(x), :] for half in range(halves)]
                at_first, at_last = lane == base + x, behind == base + x
                for half in range(halves):
                    after = jnp.where(at_first, here[half + 1] if half < last else 0.0, here[half]) + flat[old][half, plane_at(x + 1), :]
                    before = jnp.where(at_last, here[half - 1] if half > 0 else 0.0, here[half]) + flat[old][half, plane_at(x - 1), :]
                    beside = flat[old][half, plane_at(x, -1), :] + flat[old][half, plane_at(x, 1), :] + rhs[half, x]
                    beside = beside + (pltpu.roll(after, LANES - 1, 1) + pltpu.roll(before, 1, 1))
                    flat[new][half, plane_at(x), :] = KEEP * here[half] + weight[half, x] * beside

    for sweep in range(SWEEPS - 2):
        old, new = sweep % 2, (sweep + 1) % 2
        if sweep == 1:
            wait_planes(send_sem.at[0], 2 * (face + layer_planes) + 2)
            lines_of(weight, weight_y, 1)
            lines_of(rhs, rhs_y, 0)
            coefficients(0)
            coefficients(1)
        sweep_inside(old, new)
        deep = sweep == SWEEPS - 3

        wait_planes(recv_sem.at[old], 2)
        add_low = z_coef[0, 1] * pltpu.roll(z_in[old, 0], 1, 1)
        add_high = z_coef[0, 0] * pltpu.roll(z_in[old, 1], LANES - 1, 1)

        def finish(trip, faces):
            for j in range(STEP):
                x = trip * STEP + j
                at_first, at_last = lane == base + x, behind == base + x
                values = [flat[new][half, plane_at(x), :] for half in range(halves)]
                values[0] = values[0] + jnp.where(at_first, add_low, 0.0)
                values[last] = values[last] + jnp.where(at_last, add_high, 0.0)
                for half in range(halves):
                    flat[new][half, plane_at(x), :] = values[half]
                packed = pack(base + x, faces[:2], values[0], values[last])
                if deep:
                    next_low, next_high = second(base + x)
                    packed += (jnp.where(next_high, values[last], faces[2]), jnp.where(next_low, values[0], faces[3]))
                faces = packed
            return faces

        faces = list(lax.fori_loop(0, trips, finish, (nothing,) * (4 if deep else 2)))
        wait_planes(recv_sem.at[2 + old], 2 * (face + layer_planes))

        columns = [(behind, last, tall_last), (lane, 0, tall_first), (behind_two, last, tall_last_but_one), (ahead, 0, tall_second)]
        for way, turn in sides:
            x = (0, nx - 1)[way]
            late = [weight[half, x] * pltpu.roll(x_in[old, way, half], turn, 1) for half in range(halves)]
            for half in range(halves):
                flat[new][half, plane_at(x), :] += late[half]
            for i, (place, half, _) in enumerate(columns[:len(faces)]):
                faces[i] = faces[i] + jnp.where(place == base + x, late[half], 0.0)
        for i, packed in enumerate(faces):
            z_out[new, i // 2, i % 2] = packed
        for way, _ in sides:
            y = (0, ny - 1)[way]
            late = [weight_y[0, way, half] * y_in[old, way, half] for half in range(halves)]
            for half in range(halves):
                for x in range(0, nx, 8):
                    flat[new][half, row_at(x, y), :] += late[half][x:x + 8]
            for i, (_, half, mask) in enumerate(columns[:len(faces)]):
                z_out[new, i // 2, i % 2, pl.ds(y, 1)] += jnp.sum(jnp.where(mask, late[half], 0.0), axis=0, keepdims=True)
        if deep:
            deep_exchange(new)
        else:
            exchange(new)

    wait_planes(send_sem.at[1], 2 * (face + layer_planes) + 2)
    sweep_inside(0, 1)
    sweep_inside(1, 2)
    wait_planes(recv_sem.at[7], 4 * (face + layer_planes) + 4)
    wait_planes(recv_sem.at[4], 4)

    outside = (lax.rem(base + LANES - 1, LANES), lax.rem(base + nx, LANES))

    def along_plane(buf, skew, below, above, more_after=(0.0,) * halves, more_before=(0.0,) * halves):
        sums = []
        here = [buf[half, pl.ds(PAD, ny)] for half in range(halves)]
        for half in range(halves):
            after = jnp.where(lane == skew, here[half + 1] if half < last else above, here[half]) + more_after[half]
            before = jnp.where(behind == skew, here[half - 1] if half > 0 else below, here[half]) + more_before[half]
            sums.append(
                (buf[half, pl.ds(PAD - 1, ny)] + buf[half, pl.ds(PAD + 1, ny)])
                + (pltpu.roll(after, LANES - 1, 1) + pltpu.roll(before, 1, 1)))
        return sums

    def along_lines(buf, below, above):
        sums = []
        here = [buf[half, pl.ds(PAD, nx)] for half in range(halves)]
        for half in range(halves):
            after = jnp.where(tall_first, here[half + 1] if half < last else above, here[half]) + buf[half, pl.ds(PAD + 1, nx)]
            before = jnp.where(tall_last, here[half - 1] if half > 0 else below, here[half]) + buf[half, pl.ds(PAD - 1, nx)]
            sums.append(pltpu.roll(after, LANES - 1, 1) + pltpu.roll(before, 1, 1))
        return sums

    def along_columns(buf, here):
        return (buf[pl.ds(PAD - 1, ny)] + buf[pl.ds(PAD + 1, ny)]) + (pltpu.roll(here, LANES - 1, 1) + pltpu.roll(here, 1, 1))

    z_total, z_inner = [], []
    for way, turn in sides:
        back = LANES - turn
        layer = z_near[way, pl.ds(PAD, ny)]
        beyond = along_columns(z_near.at[way], layer) + z_coef_in[1, way]
        beyond = beyond + (pltpu.roll(z_far[way], turn, 1) + pltpu.roll(z_out[0, 0, 1 - way], back, 1))
        ring = pltpu.roll(KEEP * layer + z_coef_in[0, way] * beyond, turn, 1)
        late = z_coef[0, 1 - way] * pltpu.roll(layer, turn, 1)
        z_add[way, pl.ds(PAD, ny)] = late
        z_total.append(z_coef[0, 1 - way] * (ring + along_columns(z_add.at[way], late)) + KEEP * late)
        z_inner.append(z_coef[2, 1 - way] * pltpu.roll(late, turn, 1))

    def store(x, first, turn):
        eight = slice(first, first + 8)
        skew = base + x
        values = [flat[2][half, pl.ds(pl.multiple_of((x + 1) * rows, 8) + first, 8), :] for half in range(halves)]
        values[0] = values[0] + jnp.where(
            lane[eight] == skew, z_total[0][eight], jnp.where(ahead[eight] == skew, z_inner[0][eight], 0.0))
        values[last] = values[last] + jnp.where(
            behind[eight] == skew, z_total[1][eight], jnp.where(behind_two[eight] == skew, z_inner[1][eight], 0.0))
        for half in range(halves):
            out[x, eight, half * LANES:(half + 1) * LANES] = pltpu.roll(values[half], turn, 1)

    middle = range(8, ny - 8, 8)

    @pl.loop(0, (nx - 4) // INNER)
    def _(trip):
        for j in range(INNER):
            x = trip * INNER + j + 2
            for first in middle:
                store(x, first, LANES - base - x)

    wait_planes(recv_sem.at[6], 4 * (face + layer_planes))
    for way, turn in sides:
        back = LANES - turn
        edge_x, edge_y = (0, nx - 1)[way], (0, ny - 1)[way]
        inner_x, inner_y = (1, nx - 2)[way], (1, ny - 2)[way]

        beyond = [x_far[way, half] for half in range(halves)]
        own = [flat[0][half, plane_at(edge_x), :] for half in range(halves)]
        ring = along_plane(
            x_near.at[way], outside[way], 0.0, 0.0, *((own, beyond) if way == 0 else (beyond, own)))
        for half in range(halves):
            layer = x_near[way, half, pl.ds(PAD, ny)]
            ring[half] = pltpu.roll(KEEP * layer + x_coef[0, way, half] * (ring[half] + x_coef[1, way, half]), turn, 1)
            x_add[way, half, pl.ds(PAD, ny)] = weight[half, edge_x] * pltpu.roll(layer, turn, 1)
        spread = along_plane(x_add.at[way], base + edge_x, 0.0, 0.0)
        for half in range(halves):
            late = x_add[way, half, pl.ds(PAD, ny)]
            flat[2][half, plane_at(edge_x), :] += weight[half, edge_x] * (ring[half] + spread[half]) + KEEP * late
            flat[2][half, plane_at(inner_x), :] += weight[half, inner_x] * pltpu.roll(late, turn, 1)

        ring = along_lines(y_near.at[way], 0.0, 0.0)
        for half in range(halves):
            layer = y_near[way, half, pl.ds(PAD, nx)]
            own = jnp.concatenate([flat[0][half, row_at(x, edge_y), :] for x in range(0, nx, 8)], axis=0)
            beyond = ring[half] + y_coef[1, way, half] + (y_far[way, half] + own)
            ring[half] = KEEP * layer + y_coef[0, way, half] * beyond
            y_add[way, half, pl.ds(PAD, nx)] = weight_y[0, way, half] * layer
        spread = along_lines(y_add.at[way], 0.0, 0.0)
        for half in range(halves):
            late = y_add[way, half, pl.ds(PAD, nx)]
            outer = weight_y[0, way, half] * (ring[half] + spread[half]) + KEEP * late
            inner = weight_y[1, way, half] * late
            for x in range(0, nx, 8):
                flat[2][half, row_at(x, edge_y), :] += outer[x:x + 8]
                flat[2][half, row_at(x, inner_y), :] += inner[x:x + 8]

    xy_factor, xz_factor, yz_factor = {}, {}, {}
    for way, turn in sides:
        edge_x, edge_y = (0, nx - 1)[way], (0, ny - 1)[way]
        for other, other_turn in sides:
            half = (0, last)[other]
            y = (0, ny - 1)[other]
            for each in range(halves):
                through = pltpu.roll(x_coef[0, way, each, pl.ds(y, 1)], turn, 1) + y_coef[0, other, each, pl.ds(edge_x, 1)]
                xy_factor[way, other, each] = weight_y[0, other, each, pl.ds(edge_x, 1)] * through
            through = pltpu.roll(x_coef[0, way, half], turn, 1) + pltpu.roll(z_coef_in[0, other], other_turn, 1)
            xz_factor[way, other] = weight[half, edge_x] * through
            through = y_coef[0, way, half] + pltpu.roll(z_coef_in[0, other, pl.ds(edge_y, 1)], other_turn, 1)
            yz_factor[way, other] = jnp.where(
                (tall_first, tall_last)[other], weight_y[0, way, half] * through, 0.0)

    wait_planes(recv_sem.at[8], 4)
    wait_lines(recv_sem.at[5], 4 * halves + 4)
    for way, turn in sides:
        edge_x, edge_y = (0, nx - 1)[way], (0, ny - 1)[way]
        for other, other_turn in sides:
            half = (0, last)[other]
            y = (0, ny - 1)[other]
            for each in range(halves):
                line = pltpu.roll(xy_in[way, other, each, pl.ds(0, 1)], turn, 1)
                flat[2][each, pl.ds((edge_x + 1) * rows + y, 1), :] += xy_factor[way, other, each] * line
            column = pltpu.roll(xz_in[way, other], (turn + other_turn) % LANES, 1)
            at_edge = (lane, behind)[other] == base + edge_x
            flat[2][half, plane_at(edge_x), :] += jnp.where(at_edge, xz_factor[way, other] * column, 0.0)
            line = pltpu.roll(yz_in[way, other, pl.ds(0, 1)], other_turn, 1)
            through = yz_factor[way, other] * line
            for x in range(0, nx, 8):
                flat[2][half, row_at(x, edge_y), :] += through[x:x + 8]

    for x in (0, 1, nx - 2, nx - 1):
        for first in middle:
            store(x, first, LANES - base - x if x else lax.rem(LANES - base, LANES))

    @pl.loop(0, nx // OUTER)
    def _(trip):
        for j in range(OUTER):
            x = trip * OUTER + j
            for first in (0, ny - 8):
                store(x, first, LANES - base - x if j else lax.rem(LANES - base - x, LANES))

    wait_planes(send_sem.at[4], 4 * (face + layer_planes) + 4)
    wait_planes(send_sem.at[2], 4 * (face + layer_planes) + 8)
    wait_lines(send_sem.at[3], 4 * halves + 4)


def relax(initial, right_side, shift_field):
    nx, ny, nz = initial.shape
    halves = nz // LANES
    plane, padded = (ny, LANES), (ny + 2 * PAD, LANES)
    layer = (nx, LANES)
    field = (halves, nx + 2, ny + PAD, LANES)
    shapes = [
        field, field, field, (halves, nx) + plane, (halves, nx) + plane, (2, 2, halves) + layer, (1, 2, halves) + layer,
        (3, 2) + plane, (2, 2, 2) + plane,
        (2, 2, halves) + plane, (2, 2, halves) + layer, (2, 2) + plane,
        (2, halves) + padded, (2, halves) + plane, (2, halves, nx + 2 * PAD, LANES), (2, halves) + layer, (2,) + padded, (2,) + plane,
        (2, 2, halves, PAD, LANES), (2, 2) + plane, (2, 2, PAD, LANES),
        (2, 2, halves) + plane, (2, 2, halves) + layer, (2, 2) + plane,
        (2, halves) + padded, (2, halves, nx + 2 * PAD, LANES), (2,) + padded,
    ]
    dma = pltpu.SemaphoreType.DMA
    return pl.pallas_call(
        kernel,
        out_shape=jax.ShapeDtypeStruct(initial.shape, jnp.float32),
        in_specs=[pl.BlockSpec(memory_space=pltpu.HBM)] * 3,
        out_specs=pl.BlockSpec(memory_space=pltpu.VMEM),
        scratch_shapes=[pltpu.VMEM(shape, jnp.float32) for shape in shapes]
        + [dma((nx // STEP + 2,)), dma((5,)), dma((9,))],
        compiler_params=pltpu.CompilerParams(collective_id=0, has_side_effects=True, vmem_limit_bytes=32 * 2**20),
    )(*(pltpu.with_memory_space_constraint(a, pltpu.HBM) for a in (initial, right_side, shift_field)))


def solution(mesh):
    return jax.shard_map(
        relax,
        mesh=mesh,
        in_specs=(P(*AXES), P(*AXES), P(*AXES)),
        out_specs=P(*AXES),
        check_vma=False,
    )
```
